128 devices in a mesh: seq: 8 (over z, core), head: 16 (over x, y).
Axes of the slice: x: 4, y: 4, z: 4, core: 2. Of those that a mesh axis runs over, the one named last changes fastest.
Arguments:
- lengths: int32 [16], replicated, may hold values from 128 to 8192, as said below
- page_owner: int32 [1536], replicated, may hold values from 0 to 16, as said below
- page_index: int32 [1536], replicated, may hold values from 0 to 127, as said below
- page_dest: int32 [1536], replicated, may hold values from 0 to 1535, as said below
- src_cache: bfloat16 [1536, 8, 64, 256], P(('seq', 'head')), may hold values from -8 to 8
- queries: bfloat16 [2, 16, 4096], replicated, may hold values from -8 to 8
- new_kv: bfloat16 [2, 16, 8, 256], replicated, may hold values from -6 to 6
- hidden_in: bfloat16 [2, 16, 4096], P(None, None, ('seq', 'head')), may hold values from -60 to 60
- out_weight: bfloat16 [4096, 4096], P(None, ('seq', 'head')), may hold values from -1.5 to 1.5
- norm_gain: bfloat16 [4096], P(('seq', 'head')), may hold values from 0.099609375 to 1.8984375
- router: bfloat16 [4096, 8], P(('seq', 'head')), may hold values from -0.09375 to 0.09375
- routes: int32 [2, 16, 2], replicated, may hold values from 0 to 7, all different within a row
- w_gate: bfloat16 [8, 4096, 8192], P('seq', None, 'head'), may hold values from -0.09375 to 0.09375
- w_up: bfloat16 [8, 4096, 8192], P('seq', None, 'head'), may hold values from -0.09375 to 0.09375
- w_down: bfloat16 [8, 8192, 4096], P('seq', 'head'), may hold values from -0.0625 to 0.0625
Outputs:
- page_pool: bfloat16 [16, 768, 64, 256], P('head', 'seq')
- mixed: bfloat16 [2, 16, 4096], P(None, None, ('seq', 'head'))
The draws below stay inside these ranges and needn't reach their ends.
Inputs may be any that keep to these rules, and one draw needn't show every extreme that they name: Each length is at least 128; one equals 8192; the requests' pages, lengths[r] / 64 rounded up for request r, fit into the 1536 pages. `page_owner`: request r owns exactly lengths[r] / 64 rounded up source pages; the other pages carry 16. `page_index`: the pages of request r carry 0 to their count minus 1, each once; pages without request carry 0. `page_dest`: A permutation. Slot g belongs to destination group ((g % 768) // 96) * 2 + g // 768. Of the 12 pages that one device holds (pages i * 12 to (i + 1) * 12 - 1), at most 1 go to one group, and every draw has a device that sends exactly 1 to some group.
All inputs are finite; a program needn't handle non-finite values.
Results may differ from the reference program's by a relative error of at most 0.009.
Values may be sent and summed in bfloat16 or wider, within the bound.
A program may use at most 128 MiB of HBM per device.

```python
import math
import jax
import jax.numpy as jnp
from jax import lax

D = 4096
HQ = 32
KVH = 8
HD = 128
EXPERTS = 8
TOPK = 2
FF = 8192
PAGE = 64
MAXLEN = 8192
REQS = 16
STEPS = 2
PG_DEV = 12
NPAGES = 1536
SLOTS = 768
SLOTS_DEV = 96
N_SEQ = 8
N_HEAD = 16


def page_plan(base_key):
    folded = jax.random.fold_in(base_key, 9001)
    subkeys = jax.random.split(folded, 5)
    raw_lengths = jax.random.randint(subkeys[0], (REQS,), 1, MAXLEN + 1)
    spare_room = (NPAGES - 3 * REQS) * PAGE - MAXLEN
    factor = (jnp.sum(raw_lengths) + spare_room - 1) // spare_room
    lengths = jnp.minimum(2 * PAGE + raw_lengths // factor, MAXLEN)
    longest = jax.random.randint(subkeys[1], (), 0, REQS)
    request_ids = jnp.arange(REQS, dtype=jnp.int32)
    lengths = jnp.where(request_ids == longest, MAXLEN, lengths).astype(jnp.int32)
    counts = (lengths + PAGE - 1) // PAGE
    page_ends = jnp.cumsum(counts)
    starts = page_ends - counts
    logical = jnp.arange(NPAGES, dtype=jnp.int32)
    owners = jnp.sum((logical[:, None] >= page_ends[None, :]).astype(jnp.int32), axis=1)
    first_page = jnp.sum(jnp.where(owners[:, None] == request_ids[None, :], starts[None, :], 0), axis=1)
    positions = jnp.where(owners < REQS, logical - first_page, 0)
    placed = jax.random.permutation(subkeys[2], NPAGES)
    page_owner = owners[placed].astype(jnp.int32)
    page_index = positions[placed].astype(jnp.int32)
    replicas = N_HEAD // KVH
    groups = N_SEQ * replicas
    shifts = jax.random.permutation(subkeys[3], groups)
    device = logical // PG_DEV
    target = (logical % PG_DEV + shifts[device % groups]) % groups
    onehot = (target[:, None] == jnp.arange(groups, dtype=jnp.int32)[None, :]).astype(jnp.int32)
    ranking = jnp.sum((jnp.cumsum(onehot, axis=0) - onehot) * onehot, axis=1)
    spot_order = jax.random.permutation(subkeys[4], SLOTS_DEV)[ranking]
    page_dest = target % replicas * SLOTS + target // replicas * SLOTS_DEV + spot_order
    return (lengths, page_owner, page_index, page_dest.astype(jnp.int32))


def draw_lengths(key, part):
    return page_plan(key)[0]


def draw_page_owner(key, part):
    return page_plan(key)[1]


def draw_page_index(key, part):
    return page_plan(key)[2]


def draw_page_dest(key, part):
    return page_plan(key)[3]


def draw_src_cache(key, part):
    full_shape = (NPAGES, KVH, PAGE, 2 * HD)
    values = jnp.clip(jax.random.normal(key, full_shape, jnp.float32), -6.0, 6.0)
    return values.astype(jnp.bfloat16)


def draw_queries(key, part):
    full_shape = (STEPS, REQS, HQ * HD)
    values = jnp.clip(jax.random.normal(key, full_shape, jnp.float32), -6.0, 6.0)
    return values.astype(jnp.bfloat16)


def draw_hidden_in(key, part):
    full_shape = (STEPS, REQS, D)
    subkeys = jax.random.split(key, 3)
    scales = jnp.exp(jax.random.uniform(subkeys[0], (STEPS, REQS, 1), jnp.float32, 0.0, math.log(10.0)))
    values = jnp.clip(jax.random.normal(subkeys[2], full_shape, jnp.float32), -6.0, 6.0) * scales
    return values.astype(jnp.bfloat16)


def steps_of(key, dims, cuts, low, largest):
    def one(position, parts):
        draws = jax.random.uniform(jax.random.fold_in(jax.random.fold_in(key, 6), position), (parts,), jnp.float32, low / len(cuts), largest / len(cuts))
        return jnp.repeat(jnp.exp(draws), dims[position] // parts).reshape((-1,) + (1,) * (len(dims) - position - 1))

    loudness = one(*cuts[0])
    for cut in cuts[1:]:
        loudness = loudness * one(*cut)
    return loudness


def picks_of(stream_key, rows, number_of, top, lift):
    order = jax.random.permutation(jax.random.fold_in(stream_key, 1), number_of)
    favour = order
    for power in range(3):
        favour = favour * favour // number_of
    favour = favour * lift // number_of
    lots = jax.random.randint(jax.random.fold_in(stream_key, 2), (rows, number_of), 0, 4096) + favour
    sure = jax.random.permutation(jax.random.fold_in(stream_key, 3), rows)[jnp.arange(number_of) % rows]
    lots = jnp.where(jnp.arange(rows)[:, None] == sure[None, :], 1 << 14, lots)
    score = lots * number_of + jnp.arange(number_of)
    return lax.top_k(score.astype(jnp.int32), top)[1].astype(jnp.int32)


def bell_draw(key, shape, scale, most, cuts=(), kind=jnp.bfloat16):
    values = scale * jax.random.normal(key, shape, jnp.float32)
    if cuts:
        values = values * steps_of(key, shape, cuts, -0.22, 0.18)
    return jnp.clip(values, -most, most).astype(kind)


def setup_inputs(seed: int = 0) -> dict:
    keys = jax.random.split(jax.random.key(seed), 16)
    return {
        "lengths": draw_lengths(jax.random.fold_in(keys[15], 71), 0),
        "page_owner": draw_page_owner(jax.random.fold_in(keys[15], 71), 0),
        "page_index": draw_page_index(jax.random.fold_in(keys[15], 71), 0),
        "page_dest": draw_page_dest(jax.random.fold_in(keys[15], 71), 0),
        "src_cache": draw_src_cache(jax.random.fold_in(keys[15], 71), 0),
        "queries": draw_queries(jax.random.fold_in(keys[15], 71), 0),
        "new_kv": bell_draw(keys[6], (STEPS, REQS, KVH, 2 * HD), 1.0, 6.0),
        "hidden_in": draw_hidden_in(jax.random.fold_in(keys[15], 71), 0),
        "out_weight": bell_draw(keys[8], (HQ * HD, D), (HQ * HD // 256) ** -0.5, 1.5, ((1, 128),)),
        "norm_gain": jnp.clip(1.0 + 0.18 * jax.random.normal(keys[9], (D,), jnp.float32), 0.099609375, 1.8984375).astype(jnp.bfloat16),
        "router": bell_draw(keys[10], (D, EXPERTS), D ** -0.5, 0.09375, ((0, 128),)),
        "routes": picks_of(keys[11], STEPS * REQS, EXPERTS, TOPK, 2048).reshape((STEPS, REQS, TOPK)),
        "w_gate": bell_draw(keys[12], (EXPERTS, D, FF), D ** -0.5, 0.09375, ((0, 8), (2, 16))),
        "w_up": bell_draw(keys[13], (EXPERTS, D, FF), D ** -0.5, 0.09375, ((0, 8), (2, 16))),
        "w_down": bell_draw(keys[14], (EXPERTS, FF, D), FF ** -0.5, 0.0625, ((0, 8), (1, 16))),
    }


NEG_FILL = -1e+30
EPSILON = 1e-05
HIGHEST = lax.Precision.HIGHEST

def gate_mix(logits, picked):
    expert_ids = jnp.arange(logits.shape[1], dtype=jnp.int32)[None, :]
    first_hit = picked[:, 0:1] == expert_ids
    second_hit = picked[:, 1:2] == expert_ids
    first_logit = lax.optimization_barrier(jnp.sum(jnp.where(first_hit, logits, 0.0), axis=1))
    second_logit = lax.optimization_barrier(jnp.sum(jnp.where(second_hit, logits, 0.0), axis=1))
    leading = 1.0 / (1.0 + jnp.exp(second_logit - first_logit))
    trailing = 1.0 / (1.0 + jnp.exp(first_logit - second_logit))
    return jnp.where(first_hit, leading[:, None], 0.0) + jnp.where(second_hit, trailing[:, None], 0.0)

def attend(lengths, page_owner, page_index, src_cache, queries, new_kv):
    step_count = queries.shape[0]
    group_size = HQ // KVH
    grouped = queries.astype(jnp.float32).reshape(step_count, REQS, KVH, group_size, HD)
    score_scale = HD ** (-0.5)
    clipped = jnp.minimum(page_owner, REQS - 1).astype(jnp.int32)
    offsets = page_index[:, None] * PAGE + jnp.arange(PAGE, dtype=jnp.int32)[None, :]
    is_live = (page_owner < REQS)[:, None] & (offsets < jnp.take(lengths, clipped)[:, None])
    asked_rows = jnp.take(grouped, clipped, axis=1)
    key_float = src_cache[..., :HD].astype(jnp.float32)
    scores = jnp.einsum('spkgd,pktd->spkgt', asked_rows, key_float, precision=HIGHEST) * score_scale
    live_mask = is_live[None, :, None, None, :]
    scores = jnp.where(live_mask, scores, NEG_FILL)
    members = page_owner[:, None] == jnp.arange(REQS, dtype=jnp.int32)[None, :]
    page_top = lax.optimization_barrier(jnp.max(scores, axis=4))
    row_top = lax.optimization_barrier(jnp.max(jnp.where(members[None, :, :, None, None], page_top[:, :, None], NEG_FILL), axis=1))
    fresh_keys = new_kv[..., :HD].astype(jnp.float32)
    fresh_values = new_kv[..., HD:].astype(jnp.float32)
    fresh_scores = jnp.einsum('srkgd,urkd->srkgu', grouped, fresh_keys, precision=HIGHEST) * score_scale
    causal = jnp.arange(step_count)[:, None] >= jnp.arange(step_count)[None, :]
    causal_mask = causal[:, None, None, None, :]
    fresh_scores = jnp.where(causal_mask, fresh_scores, NEG_FILL)
    row_top = jnp.maximum(row_top, lax.optimization_barrier(jnp.max(fresh_scores, axis=4)))
    weights = jnp.where(live_mask, jnp.exp(scores - jnp.take(row_top, clipped, axis=1)[..., None]), 0.0)
    fresh_weights = jnp.where(causal_mask, jnp.exp(fresh_scores - row_top[..., None]), 0.0)
    member_mask = members.astype(jnp.float32)
    totals = jnp.einsum('pr,spkg->srkg', member_mask, lax.optimization_barrier(jnp.sum(weights, axis=4)), precision=HIGHEST)
    totals = totals + lax.optimization_barrier(jnp.sum(fresh_weights, axis=4))
    rounded = lax.optimization_barrier(weights.astype(jnp.bfloat16)).astype(jnp.float32)
    page_out = jnp.einsum('spkgt,pktd->spkgd', rounded, src_cache[..., HD:].astype(jnp.float32), precision=HIGHEST)
    weighted = jnp.einsum('pr,spkgd->srkgd', member_mask, page_out, precision=HIGHEST)
    fresh_rounded = lax.optimization_barrier(fresh_weights.astype(jnp.bfloat16)).astype(jnp.float32)
    weighted = weighted + jnp.einsum('srkgu,urkd->srkgd', fresh_rounded, fresh_values, precision=HIGHEST)
    return (weighted / totals[..., None]).reshape(step_count, REQS, HQ * HD).astype(jnp.bfloat16)

def reference(lengths, page_owner, page_index, page_dest, src_cache, queries, new_kv, hidden_in, out_weight, norm_gain, router, routes, w_gate, w_up, w_down):
    replicas = N_HEAD // KVH
    slot_count = NPAGES // replicas
    inverse = jnp.argsort(page_dest).astype(jnp.int32)
    ordered = jnp.take(src_cache, inverse, axis=0)
    page_pool = ordered.reshape(replicas, slot_count, KVH, PAGE, 2 * HD).transpose(2, 0, 1, 3, 4)
    page_pool = page_pool.reshape(KVH * replicas, slot_count, PAGE, 2 * HD)
    attended = attend(lengths, page_owner, page_index, src_cache, queries, new_kv)
    step_count = queries.shape[0]
    row_count = step_count * REQS
    attn_out = jnp.dot(attended.reshape(row_count, HQ * HD), out_weight, preferred_element_type=jnp.float32)
    middle = hidden_in.reshape(row_count, D).astype(jnp.float32) + attn_out
    inverse_rms = lax.rsqrt(lax.optimization_barrier(jnp.mean(middle * middle, axis=1, keepdims=True)) + EPSILON)
    normed = middle * inverse_rms * norm_gain.astype(jnp.float32)[None, :]
    logits = jnp.dot(normed, router.astype(jnp.float32), precision=HIGHEST)
    mixture = gate_mix(logits, routes.reshape(row_count, TOPK))
    features = normed.astype(jnp.bfloat16)

    def one_expert(running, expert):
        gate_act = jnp.dot(features, w_gate[expert], preferred_element_type=jnp.float32)
        upward = jnp.dot(features, w_up[expert], preferred_element_type=jnp.float32)
        inner_act = (jax.nn.silu(gate_act) * upward).astype(jnp.bfloat16)
        produced = jnp.dot(inner_act, w_down[expert], preferred_element_type=jnp.float32)
        expert_share = lax.optimization_barrier(jnp.sum(jnp.where(jnp.arange(EXPERTS, dtype=jnp.int32)[None, :] == expert, mixture, 0.0), axis=1))
        return (running + expert_share[:, None] * produced, None)
    moe_out, unused = lax.scan(one_expert, jnp.zeros((row_count, D), jnp.float32), jnp.arange(EXPERTS, dtype=jnp.int32))
    mixed = (middle + moe_out).astype(jnp.bfloat16).reshape(step_count, REQS, D)
    return (page_pool, mixed)
```

```python
import functools

import jax
import jax.numpy as jnp
from jax import lax
from jax.experimental import pallas as pl
from jax.experimental.pallas import tpu as pltpu
from jax.sharding import PartitionSpec as P

D = 4096
HQ = 32
KVH = 8
GROUP = HQ // KVH
HD = 128
EXPERTS = 8
PAGE = 64
REQS = 16
ROWS = 32
FF_DEV = 512
PG_DEV = 12
SLOTS = 768
SLOTS_DEV = 96
N_SEQ = 8
N_HEAD = 16
N_DEV = N_SEQ * N_HEAD
NEG_FILL = -1e30
EPSILON = 1e-05
HIGHEST = lax.Precision.HIGHEST
SCALE = HD ** (-0.5)
SEQ_HEAD = ("seq", "head")
BF16 = jnp.bfloat16
F32 = jnp.float32
BULK_STARTS = (0, 40, 20, 20, 20, 27)


def iota(shape, dim):
    return lax.broadcasted_iota(jnp.int32, shape, dim)


def dot(a, b, precision=None):
    return jnp.dot(a, b, preferred_element_type=F32, precision=precision)


def decode_kernel(
    lengths,
    page_owner,
    page_index,
    page_dest,
    src_hbm,
    queries_hbm,
    own_query,
    own_fresh,
    hidden,
    wo_hbm,
    gain,
    router,
    routes,
    wg_hbm,
    wu_hbm,
    wd_hbm,
    arrived,
    mixed,
    src,
    packed,
    queries,
    wo,
    wg,
    wu,
    wd,
    rs1_send,
    rs1_recv,
    ag1_send,
    ag1_recv,
    attended,
    ag2_send,
    ag2_recv,
    features,
    rs2_send,
    rs2_recv,
    src_sem,
    query_sem,
    weight_sem,
    own_sem,
    send_sem,
    recv_sem,
):
    seq = lax.axis_index("seq")
    head = lax.axis_index("head")
    me = seq * N_HEAD + head
    seqs = [lax.rem(seq + t, N_SEQ) for t in range(N_SEQ)]
    heads = [lax.rem(head + u, N_HEAD) for u in range(N_HEAD)]
    z, core, x, y = seq // 2, lax.rem(seq, 2), head // 4, lax.rem(head, 4)
    zs = [lax.rem(z + t, 4) for t in range(4)]
    cores = [lax.rem(core + t, 2) for t in range(2)]
    xs = [lax.rem(x + t, 4) for t in range(4)]
    ys = [lax.rem(y + t, 4) for t in range(4)]

    def page_copy(t):
        return pltpu.make_async_copy(src_hbm.at[:, seqs[t]], src.at[:, seqs[t]], src_sem.at[t])

    query_copy = pltpu.make_async_copy(queries_hbm, queries, query_sem)
    query_copy.start()
    for t in range(N_SEQ):
        page_copy(t).start()
    weight_copies = [
        pltpu.make_async_copy(a, b, weight_sem.at[n])
        for n, (a, b) in enumerate(((wo_hbm, wo), (wg_hbm, wg), (wu_hbm, wu), (wd_hbm, wd)))
    ]
    for copy in weight_copies:
        copy.start()

    barrier = pltpu.get_barrier_semaphore()

    def each_peer(act):
        for u in range(1, N_HEAD):
            act(seq, heads[u])

        def step(t, carry):
            to_seq = lax.rem(seq + t, N_SEQ)
            for u in range(N_HEAD):
                act(to_seq, heads[u])
            return carry

        lax.fori_loop(1, N_SEQ, step, 0)

    def greet(to_seq, to_head):
        pl.semaphore_signal(
            barrier,
            inc=1,
            device_id=(to_seq, to_head),
            device_id_type=pl.DeviceIdType.MESH,
        )

    each_peer(greet)

    def remote(source, target, phase, to_seq, to_head):
        return pltpu.make_async_remote_copy(
            src_ref=source,
            dst_ref=target,
            send_sem=send_sem.at[phase],
            recv_sem=recv_sem.at[phase],
            device_id=(to_seq, to_head),
            device_id_type=pl.DeviceIdType.MESH,
        )

    def all_but_one(buffer, phase):
        rest = buffer.at[pl.ds(0, N_DEV - 1)]
        return remote(rest, rest, phase, seq, head)

    lane = iota((1, PG_DEV * PAGE), 1)
    token_owner = jnp.full((1, PG_DEV * PAGE), REQS, jnp.int32)
    for p in range(PG_DEV):
        owner = page_owner[me * PG_DEV + p]
        limit = lengths[jnp.minimum(owner, REQS - 1)] - page_index[me * PG_DEV + p] * PAGE
        inside = (lane >= p * PAGE) & (lane < p * PAGE + jnp.minimum(limit, PAGE))
        token_owner = jnp.where(inside, owner, token_owner)

    def pack_pages():
        groups = []
        for p in range(PG_DEV):
            dest = page_dest[me * PG_DEV + p]
            upper = jnp.where(dest >= SLOTS, 1, 0)
            within = dest - upper * SLOTS
            target = jnp.int32(0)
            for n in range(1, N_SEQ):
                target = target + jnp.where(within >= n * SLOTS_DEV, 2, 0)
            groups.append(target + upper)

        def one(group, carry):
            page = jnp.int32(0)
            for p in range(PG_DEV):
                page = jnp.where(groups[p] == group, p, page)
            for k in range(KVH):
                packed[group, k] = src[page, k]
            return carry

        lax.fori_loop(0, 2 * N_SEQ, one, 0)

    started = [1]

    def start_bulk(count):
        for i in range(started[0], started[0] + count):
            j = (i * 37) % N_DEV
            to_seq = zs[j // 32] * 2 + cores[(j // 16) % 2]
            to_head = xs[(j // 4) % 4] * 4 + ys[j % 4]
            group = to_seq * 2 + lax.rem(to_head, 2)
            remote(packed.at[group, to_head // 2], arrived.at[me], 4, to_seq, to_head).start()
        started[0] += count

    query_copy.wait()
    row_request = lax.rem(iota((4 * ROWS, 1), 0), REQS)
    live = token_owner == row_request
    lane128 = iota((4 * ROWS, HD), 1)

    def attend_head(t):
        k = seqs[t]
        page_copy(t).wait()
        asked = jnp.concatenate(
            [
                queries[:, pl.ds(pl.multiple_of((k * GROUP + g) * HD, HD), HD)]
                for g in range(GROUP)
            ],
            axis=0,
        )
        keys = src[:, k, :, :HD].reshape(PG_DEV * PAGE, HD)
        values = src[:, k, :, HD:].reshape(PG_DEV * PAGE, HD)
        scores = (
            lax.dot_general(asked, keys, (((1,), (1,)), ((), ())), preferred_element_type=F32)
            * SCALE
        )
        scores = jnp.where(live, scores, NEG_FILL)
        top = jnp.max(scores, axis=1, keepdims=True)
        shift = jnp.where(top > -1e29, jnp.ceil(top * 0.25) * 4.0, NEG_FILL)
        weights = jnp.where(live, jnp.exp(scores - shift), 0.0)
        total = jnp.sum(weights, axis=1, keepdims=True)
        weighted = dot(weights.astype(BF16), values)
        total_high = total.astype(BF16).astype(F32)
        stats = jnp.where(
            lane128 < 32, shift, jnp.where(lane128 < 64, total_high, total - total_high)
        )
        parts = jnp.concatenate(
            [weighted.reshape(16, 8, HD), stats.reshape(16, 8, HD)], axis=1
        ).astype(BF16)
        rs1_send[pl.ds(k * N_HEAD, N_HEAD)] = parts

    def send_parts(t):
        for u in range(N_HEAD):
            if t or u:
                slot = seqs[t] * N_HEAD + heads[u]
                remote(rs1_send.at[slot], rs1_recv.at[me], 0, seqs[t], heads[u]).start()

    attend_head(0)
    rs1_recv[me] = rs1_send[me]
    attend_head(1)
    pl.semaphore_wait(barrier, N_DEV - 1)
    send_parts(0)
    send_parts(1)
    for t in range(2, N_SEQ):
        attend_head(t)
        send_parts(t)
    pack_pages()
    own_slot = pltpu.make_async_copy(
        packed.at[seq * 2 + lax.rem(head, 2), head // 2], arrived.at[me], own_sem
    )
    own_slot.start()
    start_bulk(BULK_STARTS[1])

    all_but_one(rs1_recv, 0).wait_recv()
    received = rs1_recv[...].astype(F32)
    outs, stats = received[:, :8], received[:, 8:]
    query = own_query[...]
    later = lax.rem(me, 4) >= 2
    fresh_scores = []
    for u in range(2):
        score = jnp.sum(query * own_fresh[u, :, :HD], axis=1, keepdims=True) * SCALE
        fresh_scores.append(score if u == 0 else jnp.where(later, score, NEG_FILL))
    top = jnp.max(stats, axis=0)[:, :1]
    top = jnp.maximum(top, jnp.maximum(fresh_scores[0], fresh_scores[1]))
    factor = jnp.exp(stats[:, :, :1] - top[None])
    weighted = jnp.sum(outs * factor, axis=0)
    totals = jnp.sum(stats * factor, axis=0)
    total = totals[:, 32:33] + totals[:, 64:65]
    for u in range(2):
        weight = jnp.exp(fresh_scores[u] - top)
        total = total + weight
        weighted = weighted + weight.astype(BF16).astype(F32) * own_fresh[u, :, HD:]
    part = (weighted / total).astype(BF16)
    ag1_send[...] = part
    ag1_recv[me] = part
    each_peer(lambda s, h: remote(ag1_send, ag1_recv.at[me], 1, s, h).start())
    start_bulk(BULK_STARTS[2])

    select = [
        jnp.where(iota((32, HD), 1) == iota((32, HD), 0) + q * 32, 1.0, 0.0) for q in range(4)
    ]
    weight_copies[0].wait()
    all_but_one(ag1_recv, 1).wait_recv()
    rows = ag1_recv[...].astype(F32).reshape(HQ, ROWS, HD)
    for a in range(HQ):
        attended[:, a * HD : (a + 1) * HD] = rows[a].astype(BF16)
    middle = hidden[...].astype(F32) + dot(attended[...], wo[...])
    scaled = middle * gain[...].astype(F32)
    lane32 = iota((ROWS, 32), 1)
    sums = dot(scaled, router[...].astype(F32), HIGHEST)
    square = jnp.sum(middle * middle, axis=1, keepdims=True)
    sums = jnp.where((lane32 == 0) | (lane32 == 16), square, sums)
    sums_high = sums.astype(BF16).astype(F32)
    sums = jnp.where(lane32 < 16, sums_high, sums - sums_high)

    def packed_rows(block, precision=None):
        return sum(
            dot(block[q * 8 : q * 8 + 8], select[q].astype(block.dtype), precision)
            for q in range(4)
        )

    part = jnp.concatenate(
        [packed_rows(scaled.astype(BF16)), packed_rows(sums.astype(BF16))], axis=0
    ).astype(BF16)
    ag2_send[...] = part
    ag2_recv[me] = part
    each_peer(lambda s, h: remote(ag2_send, ag2_recv.at[me], 2, s, h).start())
    start_bulk(BULK_STARTS[3])
    middle_packed = packed_rows(middle, HIGHEST)

    spread_row, spread_col = iota((HD, 512), 0), iota((HD, 512), 1)

    def spread(j):
        wanted = (spread_row // 32) * HD + j * 32 + lax.rem(spread_row, 32)
        return jnp.where(spread_col == wanted, 1.0, 0.0).astype(BF16)

    spreads = [spread(j) for j in range(4)]
    for copy in weight_copies[1:]:
        copy.wait()
    all_but_one(ag2_recv, 2).wait_recv()
    received = ag2_recv[...].astype(F32)
    blocks = received[:, :8].reshape(32, 4, 8, HD)
    ordered = sum(
        dot(blocks[:, j].reshape(256, HD).astype(BF16), spreads[j]) for j in range(4)
    )
    for n in range(32):
        features[:, n * HD : (n + 1) * HD] = jnp.concatenate(
            [ordered[n * 8 : n * 8 + 8, q * HD : (q + 1) * HD] for q in range(4)], axis=0
        ).astype(BF16)
    sums = jnp.sum(received[:, 8:], axis=0)
    fold_row, fold_col = iota((HD, HD), 0), iota((HD, HD), 1)
    folded = jnp.concatenate(
        [
            dot(
                sums,
                jnp.where(
                    (fold_row // 32 == q) & (lax.rem(fold_row, 16) == fold_col), 1.0, 0.0
                ),
                HIGHEST,
            )
            for q in range(4)
        ],
        axis=0,
    )
    inverse_rms = lax.rsqrt(folded[:, :1] / D + EPSILON)
    logits = folded * inverse_rms
    chosen = routes[...]
    first, second = chosen[:, :1], chosen[:, 1:2]
    expert_lane = iota((ROWS, HD), 1) - 1
    first_logit = jnp.sum(jnp.where(expert_lane == first, logits, 0.0), axis=1, keepdims=True)
    second_logit = jnp.sum(jnp.where(expert_lane == second, logits, 0.0), axis=1, keepdims=True)
    share = jnp.where(
        first == seq,
        1.0 / (1.0 + jnp.exp(second_logit - first_logit)),
        jnp.where(second == seq, 1.0 / (1.0 + jnp.exp(first_logit - second_logit)), 0.0),
    )
    gate = dot(features[...], wg[...]) * inverse_rms
    upward = dot(features[...], wu[...]) * inverse_rms
    inner = (gate / (1.0 + jnp.exp(-gate)) * upward).astype(BF16)
    start_bulk(BULK_STARTS[4])

    collect_row, collect_col = iota((HD, 512), 0), iota((HD, 512), 1)

    def collect(q):
        wanted = (collect_row // 32) * HD + q * 32 + lax.rem(collect_row, 32)
        return jnp.where(collect_col == wanted, 1.0, 0.0).astype(BF16)

    collects = [collect(q) for q in range(4)]
    produced = dot(inner, wd[...]) * share
    parts = sum(
        dot(
            jnp.concatenate(
                [produced[q * 8 : q * 8 + 8, n * HD : (n + 1) * HD] for n in range(32)], axis=0
            ).astype(BF16),
            collects[q],
        )
        for q in range(4)
    )
    for j in range(4):
        rs2_send[:, j] = parts[:, j * HD : (j + 1) * HD].reshape(32, 8, HD).astype(BF16)
    rs2_recv[me] = rs2_send[me // 4, lax.rem(me, 4)]

    def send_sums(to_seq, to_head):
        slot = to_seq * N_HEAD + to_head
        remote(
            rs2_send.at[slot // 4, lax.rem(slot, 4)], rs2_recv.at[me], 3, to_seq, to_head
        ).start()

    each_peer(send_sums)
    start_bulk(BULK_STARTS[5])
    all_but_one(rs2_recv, 3).wait_recv()
    mixed[...] = (middle_packed + jnp.sum(rs2_recv[...].astype(F32), axis=0)).astype(BF16)

    for buffer, phase in ((rs1_recv, 0), (ag1_recv, 1), (ag2_recv, 2), (rs2_recv, 3)):
        all_but_one(buffer, phase).wait_send()
    own_slot.wait()
    all_but_one(arrived, 4).wait_recv()
    all_but_one(arrived, 4).wait_send()


def body(
    lengths,
    page_owner,
    page_index,
    page_dest,
    src_cache,
    queries,
    new_kv,
    hidden_in,
    out_weight,
    norm_gain,
    router,
    routes,
    w_gate,
    w_up,
    w_down,
):
    seq = lax.axis_index("seq")
    head = lax.axis_index("head")
    me = seq * N_HEAD + head
    query_head, row_block = me // 4, me % 4
    own_query = lax.dynamic_slice(
        queries.reshape(ROWS, HQ * HD), (row_block * 8, query_head * HD), (8, HD)
    ).astype(F32)
    own_fresh = lax.dynamic_slice(
        new_kv, (0, row_block % 2 * 8, query_head // GROUP, 0), (2, 8, 1, 2 * HD)
    )[:, :, 0].astype(F32)
    wide_router = jnp.zeros((32, 32), F32)
    wide_router = wide_router.at[:, 1:9].set(router.astype(F32))
    wide_router = wide_router.at[:, 17:25].set(router.astype(F32))
    vmem = pl.BlockSpec(memory_space=pltpu.VMEM)
    smem = pl.BlockSpec(memory_space=pltpu.SMEM)
    hbm = pl.BlockSpec(memory_space=pl.ANY)
    arrived, mixed = pl.pallas_call(
        decode_kernel,
        out_shape=(
            jax.ShapeDtypeStruct((N_DEV, PAGE, 2 * HD), BF16),
            jax.ShapeDtypeStruct((8, HD), BF16),
        ),
        in_specs=[smem] * 4
        + [hbm, hbm, vmem, vmem, vmem, hbm, vmem, vmem, vmem, hbm, hbm, hbm],
        out_specs=(hbm, vmem),
        scratch_shapes=[
            pltpu.VMEM((PG_DEV, KVH, PAGE, 2 * HD), BF16),
            pltpu.VMEM((2 * N_SEQ, KVH, PAGE, 2 * HD), BF16),
            pltpu.VMEM((ROWS, D), BF16),
            pltpu.VMEM((D, 32), BF16),
            pltpu.VMEM((D, FF_DEV), BF16),
            pltpu.VMEM((D, FF_DEV), BF16),
            pltpu.VMEM((FF_DEV, D), BF16),
            pltpu.VMEM((N_DEV, 16, HD), BF16),
            pltpu.VMEM((N_DEV, 16, HD), BF16),
            pltpu.VMEM((8, HD), BF16),
            pltpu.VMEM((N_DEV, 8, HD), BF16),
            pltpu.VMEM((ROWS, D), BF16),
            pltpu.VMEM((16, HD), BF16),
            pltpu.VMEM((N_DEV, 16, HD), BF16),
            pltpu.VMEM((ROWS, D), BF16),
            pltpu.VMEM((32, 4, 8, HD), BF16),
            pltpu.VMEM((N_DEV, 8, HD), BF16),
            pltpu.SemaphoreType.DMA((N_SEQ,)),
            pltpu.SemaphoreType.DMA,
            pltpu.SemaphoreType.DMA((4,)),
            pltpu.SemaphoreType.DMA,
            pltpu.SemaphoreType.DMA((5,)),
            pltpu.SemaphoreType.DMA((5,)),
        ],
        compiler_params=pltpu.CompilerParams(
            collective_id=0, has_side_effects=True, vmem_limit_bytes=58 * 1024 * 1024
        ),
        name="decode",
    )(
        lengths,
        page_owner,
        page_index,
        page_dest,
        src_cache,
        queries.reshape(ROWS, HQ * HD),
        own_query,
        own_fresh,
        hidden_in.reshape(ROWS, 32),
        out_weight,
        norm_gain.reshape(1, 32),
        wide_router,
        routes.reshape(ROWS, 2),
        w_gate[0],
        w_up[0],
        w_down[0],
    )
    mixed = mixed.reshape(8, 4, 32).transpose(1, 0, 2).reshape(2, REQS, 32)
    first_slot = (head % 2) * SLOTS + seq * SLOTS_DEV
    slot_ids = first_slot + jnp.arange(SLOTS_DEV, dtype=jnp.int32)
    sources = jnp.arange(page_dest.shape[0], dtype=jnp.int32) // PG_DEV
    chosen = jnp.sum(
        jnp.where(page_dest[None, :] == slot_ids[:, None], sources[None, :], 0), axis=1
    )
    page_pool = jnp.take(arrived, chosen, axis=0)
    return (page_pool[None], mixed)


def solution(mesh):
    in_specs = (
        P(),
        P(),
        P(),
        P(),
        P(SEQ_HEAD, None, None, None),
        P(),
        P(),
        P(None, None, SEQ_HEAD),
        P(None, SEQ_HEAD),
        P(SEQ_HEAD),
        P(SEQ_HEAD, None),
        P(),
        P("seq", None, "head"),
        P("seq", None, "head"),
        P("seq", "head", None),
    )
    out_specs = (P("head", "seq", None, None), P(None, None, SEQ_HEAD))
    return jax.shard_map(body, mesh=mesh, in_specs=in_specs, out_specs=out_specs, check_vma=False)
```

```python
import functools

import jax
import jax.numpy as jnp
from jax import lax
from jax.experimental import pallas as pl
from jax.experimental.pallas import tpu as pltpu
from jax.sharding import PartitionSpec as P

D = 4096
HQ = 32
KVH = 8
GROUP = HQ // KVH
HD = 128
EXPERTS = 8
PAGE = 64
REQS = 16
ROWS = 32
FF_DEV = 512
PG_DEV = 12
SLOTS = 768
SLOTS_DEV = 96
N_SEQ = 8
N_HEAD = 16
N_DEV = N_SEQ * N_HEAD
NEG_FILL = -1e30
EPSILON = 1e-05
HIGHEST = lax.Precision.HIGHEST
SCALE = HD ** (-0.5)
SEQ_HEAD = ("seq", "head")
BF16 = jnp.bfloat16
F32 = jnp.float32
N_PLANE = 4
BULK_STARTS = ((14, 0), (14, 4), (14, 4), (5, 0), (14, 4), (4, 0), (14, 0), (48, 0))
MERGE, GATHER_A, FORWARD_A, GATHER_B, FORWARD_B, PAIR_SUMS, SUMS, BULK = range(4, 12)


def farthest_first(offsets):
    return sorted(offsets, key=lambda o: -sum(min(d, 4 - d) for d in o))


def balanced_order():
    left = [(n // 32, n // 16 % 2, n // 4 % 4, n % 4) for n in range(1, N_DEV)]
    loads, order = [0.0] * 6, []

    def added(offset):
        new = list(loads)
        for axis, d in enumerate((offset[2], offset[3], offset[0])):
            for way, amount in enumerate(((0, 1, 1, 0), (0, 0, 1, 1))):
                new[2 * axis + way] += amount[d]
        return new

    def spread(offset):
        new = added(offset)
        mean = sum(new) / 6
        return sum((n - mean) ** 2 for n in new), -sum(new)

    while left:
        best = min(left, key=spread)
        loads = added(best)
        left.remove(best)
        order.append(best)
    return order


PAGE_ORDER = balanced_order()
PLANE_OFFSETS = farthest_first([(n // 16, n // 4 % 4, n % 4) for n in range(1, 64)])


def iota(shape, dim):
    return lax.broadcasted_iota(jnp.int32, shape, dim)


def dot(a, b, precision=None):
    return jnp.dot(a, b, preferred_element_type=F32, precision=precision)


def decode_kernel(
    lengths,
    page_owner,
    page_index,
    page_dest,
    all_dests,
    src_hbm,
    queries_hbm,
    new_kv,
    hidden,
    wo_hbm,
    gain,
    router,
    routes,
    wg_hbm,
    wu_hbm,
    wd_hbm,
    arrived,
    mixed,
    chosen,
    src,
    packed,
    queries,
    wo,
    wg,
    wu,
    wd,
    rs1_send,
    rs1_pair,
    rs1_recv,
    ag1_send,
    ag1_recv,
    attended,
    ag2_send,
    ag2_recv,
    features,
    rs2_out,
    rs2_pair,
    rs2_send,
    rs2_recv,
    src_sem,
    query_sem,
    weight_sem,
    page_sem,
    send_sem,
    recv_sem,
):
    seq = lax.axis_index("seq")
    head = lax.axis_index("head")
    me = seq * N_HEAD + head
    heads = [lax.rem(head + u, N_HEAD) for u in range(N_HEAD)]
    z, core, x, y = seq // 2, lax.rem(seq, 2), head // 4, lax.rem(head, 4)
    zs = [lax.rem(z + t, 4) for t in range(4)]
    cores = [lax.rem(core + t, 2) for t in range(2)]
    xs = [lax.rem(x + t, 4) for t in range(4)]
    ys = [lax.rem(y + t, 4) for t in range(4)]
    other = 1 - core
    kv_heads = [2 * zs[t] + other for t in range(N_PLANE)] + [2 * zs[t] + core for t in range(N_PLANE)]

    def page_copy(t):
        return pltpu.make_async_copy(
            src_hbm.at[:, kv_heads[t]], src.at[:, kv_heads[t]], src_sem.at[t]
        )

    query_copy = pltpu.make_async_copy(queries_hbm, queries, query_sem)
    weight_copies = [
        pltpu.make_async_copy(a, b, weight_sem.at[n])
        for n, (a, b) in enumerate(((wo_hbm, wo), (wg_hbm, wg), (wu_hbm, wu), (wd_hbm, wd)))
    ]
    barrier = pltpu.get_barrier_semaphore()

    @jax.named_scope("greet")
    def each_peer(act):
        for dz, dx, dy in PLANE_OFFSETS:
            for to_core in (other, core):
                act(2 * zs[dz] + to_core, 4 * xs[dx] + ys[dy])
        act(2 * z + other, head)

    @jax.named_scope("each_plane")
    def each_of_core(act):
        for dz, dx, dy in PLANE_OFFSETS:
            act(zs[dz], 4 * xs[dx] + ys[dy])

    def greet(to_seq, to_head):
        pl.semaphore_signal(
            barrier,
            inc=1,
            device_id=(to_seq, to_head),
            device_id_type=pl.DeviceIdType.MESH,
        )

    for t in range(N_SEQ):
        page_copy(t).start()
    query_copy.start()
    each_peer(greet)

    def remote(source, target, phase, to_seq, to_head):
        return pltpu.make_async_remote_copy(
            src_ref=source,
            dst_ref=target,
            send_sem=send_sem.at[phase],
            recv_sem=recv_sem.at[phase],
            device_id=(to_seq, to_head),
            device_id_type=pl.DeviceIdType.MESH,
        )

    def to_other_core(source, target, phase):
        return remote(source, target, phase, 2 * z + other, head)

    def received_all(rest, phase):
        return remote(rest, rest, phase, 2 * z + other, head)

    def arrive(rest, phase):
        with jax.named_scope(f"arrive{phase}"):
            received_all(rest, phase).wait_recv()

    lane = iota((1, PG_DEV * PAGE), 1)
    token_owner = jnp.full((1, PG_DEV * PAGE), REQS, jnp.int32)
    for p in range(PG_DEV):
        owner = page_owner[me * PG_DEV + p]
        limit = lengths[jnp.minimum(owner, REQS - 1)] - page_index[me * PG_DEV + p] * PAGE
        inside = (lane >= p * PAGE) & (lane < p * PAGE + jnp.minimum(limit, PAGE))
        token_owner = jnp.where(inside, owner, token_owner)

    @jax.named_scope("pack")
    def pack_pages():
        groups = []
        for p in range(PG_DEV):
            dest = page_dest[me * PG_DEV + p]
            upper = jnp.where(dest >= SLOTS, 1, 0)
            within = dest - upper * SLOTS
            target = jnp.int32(0)
            for n in range(1, N_SEQ):
                target = target + jnp.where(within >= n * SLOTS_DEV, 2, 0)
            groups.append(target + upper)

        def one(group, carry):
            page = jnp.int32(0)
            for p in range(PG_DEV):
                page = jnp.where(groups[p] == group, p, page)
            for k in range(KVH):
                packed[group, k] = src[page, k]
            return carry

        lax.fori_loop(0, 2 * N_SEQ, one, 0)

    started, finished = [0], [0]

    def page_send(i):
        dz, dc, dx, dy = PAGE_ORDER[i]
        to_seq = zs[dz] * 2 + cores[dc]
        to_head = xs[dx] * 4 + ys[dy]
        part = packed.at[to_seq * 2 + lax.rem(to_head, 2), to_head // 2]
        return pltpu.make_async_remote_copy(
            src_ref=part,
            dst_ref=arrived.at[me],
            send_sem=page_sem.at[i],
            recv_sem=recv_sem.at[BULK],
            device_id=(to_seq, to_head),
            device_id_type=pl.DeviceIdType.MESH,
        )

    def finish_pages(count):
        while finished[0] < count:
            page_send(finished[0]).wait_send()
            finished[0] += 1

    @jax.named_scope("bulk")
    def start_bulk(point):
        count, window = BULK_STARTS[point]
        for i in range(started[0], started[0] + count):
            if window:
                finish_pages(i + 1 - window)
            page_send(i).start()
        started[0] += count

    row_request = lax.rem(iota((4 * ROWS, 1), 0), REQS)
    live = token_owner == row_request
    lane128 = iota((4 * ROWS, HD), 1)
    with jax.named_scope("pages"):
        for t in range(N_SEQ):
            page_copy(t).wait()
    query_copy.wait()
    for copy in weight_copies:
        copy.start()
    pack_pages()
    with jax.named_scope("greeted"):
        pl.semaphore_wait(barrier, N_DEV - 1)
    arrived[me] = packed[seq * 2 + lax.rem(head, 2), head // 2]
    start_bulk(0)

    @jax.named_scope("attend")
    def attend_head(t):
        k = kv_heads[t]
        asked = jnp.concatenate(
            [
                queries[:, pl.ds(pl.multiple_of((k * GROUP + g) * HD, HD), HD)]
                for g in range(GROUP)
            ],
            axis=0,
        )
        keys = src[:, k, :, :HD].reshape(PG_DEV * PAGE, HD)
        values = src[:, k, :, HD:].reshape(PG_DEV * PAGE, HD)
        scores = (
            lax.dot_general(asked, keys, (((1,), (1,)), ((), ())), preferred_element_type=F32)
            * SCALE
        )
        scores = jnp.where(live, scores, NEG_FILL)
        top = jnp.max(scores, axis=1, keepdims=True)
        shift = jnp.where(top > -1e29, jnp.ceil(top * 0.25) * 4.0, NEG_FILL)
        weights = jnp.where(live, jnp.exp(scores - shift), 0.0)
        total = jnp.sum(weights, axis=1, keepdims=True)
        weighted = dot(weights.astype(BF16), values)
        if t >= N_PLANE:
            pair = rs1_pair.at[zs[t - N_PLANE]]
            arrive(pair, t - N_PLANE)
            pair = pair[...].astype(F32)
            pair_out = pair[:, :8].reshape(4 * ROWS, HD)
            pair_stats = pair[:, 8:].reshape(4 * ROWS, HD)
            pair_shift = pair_stats[:, :1]
            pair_total = pair_stats[:, 32:33] + pair_stats[:, 64:65]
            joint = jnp.maximum(shift, pair_shift)
            factor, pair_factor = jnp.exp(shift - joint), jnp.exp(pair_shift - joint)
            total = total * factor + pair_total * pair_factor
            weighted = weighted * factor + pair_out * pair_factor
            shift = joint
        total_high = total.astype(BF16).astype(F32)
        stats = jnp.where(
            lane128 < 32, shift, jnp.where(lane128 < 64, total_high, total - total_high)
        )
        rs1_send[k] = jnp.concatenate(
            [weighted.reshape(16, 8, HD), stats.reshape(16, 8, HD)], axis=1
        ).astype(BF16)

    for t in range(N_PLANE):
        attend_head(t)
        to_other_core(rs1_send.at[kv_heads[t]], rs1_pair.at[zs[t]], t).start()
    slot = z * N_HEAD + head
    for t in range(N_PLANE, N_SEQ):
        attend_head(t)
        for u in range(N_HEAD):
            part = rs1_send.at[kv_heads[t], heads[u]]
            if t > N_PLANE or u:
                remote(part, rs1_recv.at[slot], MERGE, kv_heads[t], heads[u]).start()
            else:
                rs1_recv[slot] = part[...]
    start_bulk(1)

    slot_row, slot_lane = iota((HD, HD), 0), iota((HD, HD), 1)
    wanted_slot = slot_row + lax.rem(head, 2) * SLOTS + seq * SLOTS_DEV
    found = jnp.zeros((HD, HD), jnp.int32)
    for n in range(N_DEV * PG_DEV // HD):
        origin = (n * HD + iota((1, HD), 1)) // PG_DEV
        found = found + jnp.where(all_dests[n : n + 1] == wanted_slot, origin, 0)
    found = jnp.sum(found.astype(F32), axis=1, keepdims=True)
    found = jnp.where(slot_row == slot_lane, found, 0.0)
    chosen[...] = jnp.sum(found, axis=0, keepdims=True).astype(jnp.int32)

    block = lax.rem(me, 4)
    later = block >= 2
    column = queries[:, pl.ds(pl.multiple_of(me // 4 * HD, HD), HD)].astype(F32)
    query = column[:8]
    for n in range(1, 4):
        query = jnp.where(block == n, column[n * 8 : n * 8 + 8], query)
    kv_lane = iota((8, KVH, 2 * HD), 1)
    first_request = lax.rem(block, 2) * 8
    own_fresh = [
        jnp.sum(
            jnp.where(
                kv_lane == me // 16,
                new_kv[u, pl.ds(first_request, 8)].astype(F32),
                0.0,
            ),
            axis=1,
        )
        for u in range(2)
    ]
    fresh_scores = []
    for u in range(2):
        score = jnp.sum(query * own_fresh[u][:, :HD], axis=1, keepdims=True) * SCALE
        fresh_scores.append(score if u == 0 else jnp.where(later, score, NEG_FILL))
    arrive(rs1_recv.at[pl.ds(0, N_DEV // 2 - 1)], MERGE)
    received = rs1_recv[...].astype(F32)
    outs, stats = received[:, :8], received[:, 8:]
    top = jnp.max(stats, axis=0)[:, :1]
    top = jnp.maximum(top, jnp.maximum(fresh_scores[0], fresh_scores[1]))
    factor = jnp.exp(stats[:, :, :1] - top[None])
    weighted = jnp.sum(outs * factor, axis=0)
    totals = jnp.sum(stats * factor, axis=0)
    total = totals[:, 32:33] + totals[:, 64:65]
    for u in range(2):
        weight = jnp.exp(fresh_scores[u] - top)
        total = total + weight
        weighted = weighted + weight.astype(BF16).astype(F32) * own_fresh[u][:, HD:]
    part = (weighted / total).astype(BF16)
    ag1_send[...] = part
    ag1_recv[core, slot] = part

    def gather(part, whole, phase):
        each_of_core(
            lambda to_z, to_head: remote(
                part, whole.at[core, slot], phase, 2 * to_z + core, to_head
            ).start()
        )

    gather(ag1_send, ag1_recv, GATHER_A)
    start_bulk(2)

    select = [
        jnp.where(iota((32, HD), 1) == iota((32, HD), 0) + q * 32, 1.0, 0.0) for q in range(4)
    ]
    router_row = iota((ROWS, EXPERTS), 0)
    wide_router = dot(
        jnp.where(lax.rem(router_row, 16) == iota((ROWS, EXPERTS), 1) + 1, 1.0, 0.0).astype(BF16),
        router[...],
    )
    weight_copies[0].wait()
    def forward(whole, phase, point):
        half = whole.at[core]
        arrive(half.at[pl.ds(0, N_DEV // 2 - 1)], phase)
        to_other_core(half, half, phase + 1).start()
        start_bulk(point)
        arrive(half, phase + 1)

    forward(ag1_recv, GATHER_A, 3)
    for n in range(N_PLANE):
        for c in range(2):
            rows = ag1_recv[c, n * N_HEAD : (n + 1) * N_HEAD].astype(F32).reshape(4, ROWS, HD)
            for g in range(GROUP):
                a = (n * 2 + c) * GROUP + g
                attended[:, a * HD : (a + 1) * HD] = rows[g].astype(BF16)
    middle = hidden[...].astype(F32) + lax.dot_general(
        attended[...], wo[...], (((1,), (1,)), ((), ())), preferred_element_type=F32
    )
    scaled = middle * gain[...].astype(F32)
    lane32 = iota((ROWS, 32), 1)
    sums = lax.dot_general(
        scaled,
        wide_router,
        (((1,), (1,)), ((), ())),
        preferred_element_type=F32,
        precision=HIGHEST,
    )
    square = jnp.sum(middle * middle, axis=1, keepdims=True)
    sums = jnp.where((lane32 == 0) | (lane32 == 16), square, sums)
    sums_high = sums.astype(BF16).astype(F32)
    sums = jnp.where(lane32 < 16, sums_high, sums - sums_high)

    def packed_rows(block, precision=None):
        return sum(
            dot(block[q * 8 : q * 8 + 8], select[q].astype(block.dtype), precision)
            for q in range(4)
        )

    part = jnp.concatenate(
        [packed_rows(scaled.astype(BF16)), packed_rows(sums.astype(BF16))], axis=0
    ).astype(BF16)
    ag2_send[...] = part
    ag2_recv[core, slot] = part
    gather(ag2_send, ag2_recv, GATHER_B)
    start_bulk(4)
    middle_packed = packed_rows(middle, HIGHEST)

    spread_row, spread_col = iota((HD, 512), 0), iota((HD, 512), 1)

    def spread(j):
        wanted = (spread_row // 32) * HD + j * 32 + lax.rem(spread_row, 32)
        return jnp.where(spread_col == wanted, 1.0, 0.0).astype(BF16)

    spreads = [spread(j) for j in range(4)]
    for copy in weight_copies[1:]:
        copy.wait()
    forward(ag2_recv, GATHER_B, 5)
    start_bulk(6)
    received = ag2_recv[...].astype(F32)
    blocks = received[:, :, :8].reshape(32, 4, 8, HD)
    ordered = sum(
        dot(blocks[:, j].reshape(256, HD).astype(BF16), spreads[j]) for j in range(4)
    )
    for n in range(32):
        place = n // 4 % 4 * 8 + n // 16 * 4 + n % 4
        features[:, place * HD : (place + 1) * HD] = jnp.concatenate(
            [ordered[n * 8 : n * 8 + 8, q * HD : (q + 1) * HD] for q in range(4)], axis=0
        ).astype(BF16)
    sums = jnp.sum(jnp.sum(received[:, :, 8:], axis=1), axis=0)
    fold_row, fold_col = iota((HD, HD), 0), iota((HD, HD), 1)
    folded = jnp.concatenate(
        [
            dot(
                sums,
                jnp.where(
                    (fold_row // 32 == q) & (lax.rem(fold_row, 16) == fold_col), 1.0, 0.0
                ),
                HIGHEST,
            )
            for q in range(4)
        ],
        axis=0,
    )
    inverse_rms = lax.rsqrt(folded[:, :1] / D + EPSILON)
    logits = folded * inverse_rms
    diagonal = iota((REQS, REQS), 0) == iota((REQS, REQS), 1)

    def picked(choice):
        rows = [
            jnp.sum(
                jnp.where(diagonal, routes[s, choice : choice + 1, :].astype(F32), 0.0),
                axis=1,
                keepdims=True,
            )
            for s in range(2)
        ]
        return jnp.concatenate(rows, axis=0).astype(jnp.int32)

    first, second = picked(0), picked(1)
    expert_lane = iota((ROWS, HD), 1) - 1
    first_logit = jnp.sum(jnp.where(expert_lane == first, logits, 0.0), axis=1, keepdims=True)
    second_logit = jnp.sum(jnp.where(expert_lane == second, logits, 0.0), axis=1, keepdims=True)
    share = jnp.where(
        first == seq,
        1.0 / (1.0 + jnp.exp(second_logit - first_logit)),
        jnp.where(second == seq, 1.0 / (1.0 + jnp.exp(first_logit - second_logit)), 0.0),
    )
    gate = dot(features[...], wg[...]) * inverse_rms
    upward = dot(features[...], wu[...]) * inverse_rms
    inner = (gate / (1.0 + jnp.exp(-gate)) * upward).astype(BF16)

    collect_row, collect_col = iota((HD, 512), 0), iota((HD, 512), 1)

    def collect(q):
        wanted = (collect_row // 32) * HD + q * 32 + lax.rem(collect_row, 32)
        return jnp.where(collect_col == wanted, 1.0, 0.0).astype(BF16)

    collects = [collect(q) for q in range(4)]
    def produce(parity):
        products = [
            dot(inner, wd[:, pl.ds(pl.multiple_of((2 * n + parity) * 512, 512), 512)]) * share
            for n in range(N_PLANE)
        ]
        return sum(
            dot(
                jnp.concatenate(
                    [
                        product[q * 8 : q * 8 + 8, n * HD : (n + 1) * HD]
                        for product in products
                        for n in range(4)
                    ],
                    axis=0,
                ).astype(BF16),
                collects[q],
            )
            for q in range(4)
        )

    with jax.named_scope("down"):
        parts = produce(other)
        for j in range(4):
            rs2_out[:, j] = parts[:, j * HD : (j + 1) * HD].reshape(16, 8, HD).astype(BF16)
        to_other_core(rs2_out, rs2_pair, PAIR_SUMS).start()
        parts = produce(core)
    arrive(rs2_pair, PAIR_SUMS)
    for j in range(4):
        part = parts[:, j * HD : (j + 1) * HD].reshape(16, 8, HD)
        rs2_send[:, j] = (part + rs2_pair[:, j].astype(F32)).astype(BF16)
    rs2_recv[slot] = rs2_send[slot // 4, lax.rem(slot, 4)]

    def send_sums(to_z, to_head):
        part = rs2_send.at[to_z * 4 + to_head // 4, lax.rem(to_head, 4)]
        remote(part, rs2_recv.at[slot], SUMS, 2 * to_z + core, to_head).start()

    each_of_core(send_sums)
    start_bulk(7)
    arrive(rs2_recv.at[pl.ds(0, N_DEV // 2 - 1)], SUMS)
    mixed[...] = (middle_packed + jnp.sum(rs2_recv[...].astype(F32), axis=0)).astype(BF16)

    most = N_DEV // 2 - 1
    for t in range(N_PLANE):
        received_all(rs1_pair.at[t], t).wait_send()
    for rest, phase in (
        (rs1_recv.at[pl.ds(0, most)], MERGE),
        (ag1_recv.at[0, pl.ds(0, most)], GATHER_A),
        (ag1_recv.at[0], FORWARD_A),
        (ag2_recv.at[0, pl.ds(0, most)], GATHER_B),
        (ag2_recv.at[0], FORWARD_B),
        (rs2_pair, PAIR_SUMS),
        (rs2_recv.at[pl.ds(0, most)], SUMS),
    ):
        received_all(rest, phase).wait_send()
    arrive(arrived.at[pl.ds(0, N_DEV - 1)], BULK)
    finish_pages(N_DEV - 1)


def place_kernel(chosen, arrived, mixed_packed, pool, mixed, sem):
    for j in range(SLOTS_DEV):
        pltpu.make_async_copy(arrived.at[chosen[0, j]], pool.at[j], sem).start()
    block = mixed_packed[...].astype(F32)
    for s in range(2):
        mixed[s] = jnp.concatenate(
            [block[:, q * 32 : (q + 1) * 32] for q in (2 * s, 2 * s + 1)], axis=0
        ).astype(BF16)
    pltpu.make_async_copy(arrived.at[pl.ds(0, SLOTS_DEV)], pool, sem).wait()


def body(
    lengths,
    page_owner,
    page_index,
    page_dest,
    src_cache,
    queries,
    new_kv,
    hidden_in,
    out_weight,
    norm_gain,
    router,
    routes,
    w_gate,
    w_up,
    w_down,
):
    vmem = pl.BlockSpec(memory_space=pltpu.VMEM)
    smem = pl.BlockSpec(memory_space=pltpu.SMEM)
    hbm = pl.BlockSpec(memory_space=pltpu.HBM)
    arrived, mixed, chosen = pl.pallas_call(
        decode_kernel,
        out_shape=(
            pltpu.VMEM((N_DEV, PAGE, 2 * HD), BF16),
            pltpu.VMEM((8, HD), BF16),
            pltpu.VMEM((1, HD), jnp.int32),
        ),
        in_specs=[smem] * 4
        + [vmem, hbm, hbm, vmem, vmem, hbm, vmem, vmem, vmem, hbm, hbm, hbm],
        out_specs=(vmem, vmem, vmem),
        scratch_shapes=[
            pltpu.VMEM((PG_DEV, KVH, PAGE, 2 * HD), BF16),
            pltpu.VMEM((2 * N_SEQ, KVH, PAGE, 2 * HD), BF16),
            pltpu.VMEM((ROWS, D), BF16),
            pltpu.VMEM((32, D), BF16),
            pltpu.VMEM((D, FF_DEV), BF16),
            pltpu.VMEM((D, FF_DEV), BF16),
            pltpu.VMEM((FF_DEV, D), BF16),
            pltpu.VMEM((KVH, 16, 16, HD), BF16),
            pltpu.VMEM((N_PLANE, 16, 16, HD), BF16),
            pltpu.VMEM((N_DEV // 2, 16, HD), BF16),
            pltpu.VMEM((8, HD), BF16),
            pltpu.VMEM((2, N_DEV // 2, 8, HD), BF16),
            pltpu.VMEM((ROWS, D), BF16),
            pltpu.VMEM((16, HD), BF16),
            pltpu.VMEM((2, N_DEV // 2, 16, HD), BF16),
            pltpu.VMEM((ROWS, D), BF16),
            pltpu.VMEM((16, 4, 8, HD), BF16),
            pltpu.VMEM((16, 4, 8, HD), BF16),
            pltpu.VMEM((16, 4, 8, HD), BF16),
            pltpu.VMEM((N_DEV // 2, 8, HD), BF16),
            pltpu.SemaphoreType.DMA((N_SEQ,)),
            pltpu.SemaphoreType.DMA,
            pltpu.SemaphoreType.DMA((4,)),
            pltpu.SemaphoreType.DMA((N_DEV - 1,)),
            pltpu.SemaphoreType.DMA((12,)),
            pltpu.SemaphoreType.DMA((12,)),
        ],
        compiler_params=pltpu.CompilerParams(
            collective_id=0, has_side_effects=True, vmem_limit_bytes=59 * 1024 * 1024
        ),
        name="decode",
    )(
        lengths,
        page_owner,
        page_index,
        page_dest,
        page_dest.reshape(N_DEV * PG_DEV // HD, HD),
        src_cache,
        queries.reshape(ROWS, HQ * HD),
        new_kv,
        hidden_in.reshape(ROWS, 32),
        out_weight.T,
        norm_gain.reshape(1, 32),
        router.T,
        routes.transpose(0, 2, 1),
        w_gate[0],
        w_up[0],
        w_down[0],
    )
    page_pool, mixed = pl.pallas_call(
        place_kernel,
        out_shape=(
            jax.ShapeDtypeStruct((SLOTS_DEV, PAGE, 2 * HD), BF16),
            jax.ShapeDtypeStruct((2, REQS, 32), BF16),
        ),
        in_specs=[smem, vmem, vmem],
        out_specs=(hbm, vmem),
        scratch_shapes=[pltpu.SemaphoreType.DMA],
        compiler_params=pltpu.CompilerParams(vmem_limit_bytes=1024 * 1024),
        name="place",
    )(
        chosen,
        pltpu.with_memory_space_constraint(arrived, pltpu.VMEM),
        pltpu.with_memory_space_constraint(mixed, pltpu.VMEM),
    )
    return (page_pool[None], mixed)


def solution(mesh):
    in_specs = (
        P(),
        P(),
        P(),
        P(),
        P(SEQ_HEAD, None, None, None),
        P(),
        P(),
        P(None, None, SEQ_HEAD),
        P(None, SEQ_HEAD),
        P(SEQ_HEAD),
        P(SEQ_HEAD, None),
        P(),
        P("seq", None, "head"),
        P("seq", None, "head"),
        P("seq", "head", None),
    )
    out_specs = (P("head", "seq", None, None), P(None, None, SEQ_HEAD))
    return jax.shard_map(body, mesh=mesh, in_specs=in_specs, out_specs=out_specs, check_vma=False)
```

```python
import functools

import jax
import jax.numpy as jnp
from jax import lax
from jax.experimental import pallas as pl
from jax.experimental.pallas import tpu as pltpu
from jax.sharding import PartitionSpec as P

D = 4096
HQ = 32
KVH = 8
GROUP = HQ // KVH
HD = 128
EXPERTS = 8
PAGE = 64
REQS = 16
ROWS = 32
FF_DEV = 512
PG_DEV = 12
SLOTS = 768
SLOTS_DEV = 96
N_SEQ = 8
N_HEAD = 16
N_DEV = N_SEQ * N_HEAD
NEG_FILL = -1e30
EPSILON = 1e-05
HIGHEST = lax.Precision.HIGHEST
SCALE = HD ** (-0.5)
SEQ_HEAD = ("seq", "head")
BF16 = jnp.bfloat16
F32 = jnp.float32
N_PLANE = 4
PACED = 4
BULK_STARTS = ((14, 0), (14, 1), (14, 1), (5, 0), (14, 1), (4, 0), (28, 0), (34, 0))
MERGE, GATHER_A, FORWARD_A, GATHER_B, FORWARD_B, PAIR_SUMS, SUMS, BULK = range(4, 12)


def farthest_first(offsets):
    return sorted(offsets, key=lambda o: -sum(min(d, 4 - d) for d in o))


def balanced_order():
    left = [(n // 32, n // 16 % 2, n // 4 % 4, n % 4) for n in range(1, N_DEV)]
    loads, order = [0.0] * 6, []

    def added(offset):
        new = list(loads)
        for axis, d in enumerate((offset[2], offset[3], offset[0])):
            for way, amount in enumerate(((0, 1, 1, 0), (0, 0, 1, 1))):
                new[2 * axis + way] += amount[d]
        return new

    def spread(offset):
        new = added(offset)
        mean = sum(new) / 6
        return sum((n - mean) ** 2 for n in new), -sum(new)

    while left:
        best = min(left, key=spread)
        loads = added(best)
        left.remove(best)
        order.append(best)
    return order


PAGE_ORDER = balanced_order()
PLANE_OFFSETS = farthest_first([(n // 16, n // 4 % 4, n % 4) for n in range(1, 64)])


def iota(shape, dim):
    return lax.broadcasted_iota(jnp.int32, shape, dim)


def dot(a, b, precision=None):
    return jnp.dot(a, b, preferred_element_type=F32, precision=precision)


def decode_kernel(
    lengths_hbm,
    page_owner_hbm,
    page_index_hbm,
    page_dest_hbm,
    all_dests_hbm,
    src_hbm,
    queries_hbm,
    new_kv_hbm,
    hidden_hbm,
    wo_hbm,
    gain_hbm,
    router_hbm,
    routes_hbm,
    wg_hbm,
    wu_hbm,
    wd_hbm,
    pool,
    mixed,
    lengths,
    page_owner,
    page_index,
    page_dest,
    all_dests,
    new_kv,
    hidden,
    gain,
    router,
    routes,
    chosen,
    chosen_scalars,
    arrived,
    src,
    packed,
    queries,
    wo,
    wg,
    wu,
    wd,
    rs1_send,
    rs1_pair,
    rs1_recv,
    ag1_send,
    ag1_recv,
    attended,
    ag2_send,
    ag2_recv,
    features,
    rs2_out,
    rs2_pair,
    rs2_send,
    rs2_recv,
    small_sem,
    chosen_sem,
    src_sem,
    query_sem,
    weight_sem,
    page_sem,
    send_sem,
    recv_sem,
):
    seq = lax.axis_index("seq")
    head = lax.axis_index("head")
    me = seq * N_HEAD + head
    heads = [lax.rem(head + u, N_HEAD) for u in range(N_HEAD)]
    z, core, x, y = seq // 2, lax.rem(seq, 2), head // 4, lax.rem(head, 4)
    zs = [lax.rem(z + t, 4) for t in range(4)]
    cores = [lax.rem(core + t, 2) for t in range(2)]
    xs = [lax.rem(x + t, 4) for t in range(4)]
    ys = [lax.rem(y + t, 4) for t in range(4)]
    other = 1 - core
    kv_heads = [2 * zs[t] + other for t in range(N_PLANE)] + [2 * zs[t] + core for t in range(N_PLANE)]

    def page_copy(t):
        return pltpu.make_async_copy(
            src_hbm.at[:, kv_heads[t]], src.at[:, kv_heads[t]], src_sem.at[t]
        )

    query_copy = pltpu.make_async_copy(queries_hbm, queries, query_sem)
    weight_copies = [
        pltpu.make_async_copy(a, b, weight_sem.at[n])
        for n, (a, b) in enumerate(((wo_hbm, wo), (wg_hbm, wg), (wu_hbm, wu), (wd_hbm, wd)))
    ]
    barrier = pltpu.get_barrier_semaphore()

    @jax.named_scope("greet")
    def each_peer(act):
        for dz, dx, dy in PLANE_OFFSETS:
            for to_core in (other, core):
                act(2 * zs[dz] + to_core, 4 * xs[dx] + ys[dy])
        act(2 * z + other, head)

    @jax.named_scope("each_plane")
    def each_of_core(act):
        for dz, dx, dy in PLANE_OFFSETS:
            act(zs[dz], 4 * xs[dx] + ys[dy])

    def greet(to_seq, to_head):
        pl.semaphore_signal(
            barrier,
            inc=1,
            device_id=(to_seq, to_head),
            device_id_type=pl.DeviceIdType.MESH,
        )

    small_copies = [
        pltpu.make_async_copy(a, b, small_sem.at[n])
        for n, (a, b) in enumerate(
            (
                (lengths_hbm, lengths),
                (page_owner_hbm, page_owner),
                (page_index_hbm, page_index),
                (page_dest_hbm, page_dest),
                (all_dests_hbm, all_dests),
                (new_kv_hbm, new_kv),
                (hidden_hbm, hidden),
                (gain_hbm, gain),
                (router_hbm, router),
                (routes_hbm, routes),
            )
        )
    ]
    for t in range(N_SEQ):
        page_copy(t).start()
    for copy in small_copies:
        copy.start()
    query_copy.start()
    each_peer(greet)
    with jax.named_scope("small"):
        for copy in small_copies:
            copy.wait()

    def remote(source, target, phase, to_seq, to_head):
        return pltpu.make_async_remote_copy(
            src_ref=source,
            dst_ref=target,
            send_sem=send_sem.at[phase],
            recv_sem=recv_sem.at[phase],
            device_id=(to_seq, to_head),
            device_id_type=pl.DeviceIdType.MESH,
        )

    def to_other_core(source, target, phase):
        return remote(source, target, phase, 2 * z + other, head)

    def received_all(rest, phase):
        return remote(rest, rest, phase, 2 * z + other, head)

    def arrive(rest, phase):
        with jax.named_scope(f"arrive{phase}"):
            received_all(rest, phase).wait_recv()

    lane = iota((1, PG_DEV * PAGE), 1)
    token_owner = jnp.full((1, PG_DEV * PAGE), REQS, jnp.int32)
    for p in range(PG_DEV):
        owner = page_owner[me * PG_DEV + p]
        limit = lengths[jnp.minimum(owner, REQS - 1)] - page_index[me * PG_DEV + p] * PAGE
        inside = (lane >= p * PAGE) & (lane < p * PAGE + jnp.minimum(limit, PAGE))
        token_owner = jnp.where(inside, owner, token_owner)

    @jax.named_scope("pack")
    def pack_pages():
        groups = []
        for p in range(PG_DEV):
            dest = page_dest[me * PG_DEV + p]
            upper = jnp.where(dest >= SLOTS, 1, 0)
            within = dest - upper * SLOTS
            target = jnp.int32(0)
            for n in range(1, N_SEQ):
                target = target + jnp.where(within >= n * SLOTS_DEV, 2, 0)
            groups.append(target + upper)

        def one(group, carry):
            page = jnp.int32(0)
            for p in range(PG_DEV):
                page = jnp.where(groups[p] == group, p, page)
            for k in range(KVH):
                packed[group, k] = src[page, k]
            return carry

        lax.fori_loop(0, 2 * N_SEQ, one, 0)

    started, paced = [0], []

    def page_send(i, sem):
        dz, dc, dx, dy = PAGE_ORDER[i]
        to_seq = zs[dz] * 2 + cores[dc]
        to_head = xs[dx] * 4 + ys[dy]
        part = packed.at[to_seq * 2 + lax.rem(to_head, 2), to_head // 2]
        return pltpu.make_async_remote_copy(
            src_ref=part,
            dst_ref=arrived.at[me],
            send_sem=page_sem.at[sem],
            recv_sem=recv_sem.at[BULK],
            device_id=(to_seq, to_head),
            device_id_type=pl.DeviceIdType.MESH,
        )

    @jax.named_scope("bulk")
    def start_bulk(point):
        count, window = BULK_STARTS[point]
        for i in range(started[0], started[0] + count):
            sem = PACED + point
            if window:
                sem = len(paced) % PACED
                if len(paced) >= PACED:
                    page_send(*paced[-PACED]).wait_send()
                paced.append((i, sem))
            page_send(i, sem).start()
        started[0] += count

    def finish_pages():
        for i, sem in paced[-PACED:]:
            page_send(i, sem).wait_send()
        for point, (count, window) in enumerate(BULK_STARTS):
            if not window:
                rest = arrived.at[pl.ds(0, count)]
                pltpu.make_async_remote_copy(
                    src_ref=rest,
                    dst_ref=rest,
                    send_sem=page_sem.at[PACED + point],
                    recv_sem=recv_sem.at[BULK],
                    device_id=(2 * z + other, head),
                    device_id_type=pl.DeviceIdType.MESH,
                ).wait_send()

    row_request = lax.rem(iota((4 * ROWS, 1), 0), REQS)
    live = token_owner == row_request
    lane128 = iota((4 * ROWS, HD), 1)
    with jax.named_scope("pages"):
        for t in range(N_SEQ):
            page_copy(t).wait()
    query_copy.wait()
    for copy in weight_copies:
        copy.start()
    pack_pages()
    with jax.named_scope("greeted"):
        pl.semaphore_wait(barrier, N_DEV - 1)
    arrived[me] = packed[seq * 2 + lax.rem(head, 2), head // 2]
    start_bulk(0)

    @jax.named_scope("attend")
    def attend_head(t):
        k = kv_heads[t]
        asked = jnp.concatenate(
            [
                queries[:, pl.ds(pl.multiple_of((k * GROUP + g) * HD, HD), HD)]
                for g in range(GROUP)
            ],
            axis=0,
        )
        keys = src[:, k, :, :HD].reshape(PG_DEV * PAGE, HD)
        values = src[:, k, :, HD:].reshape(PG_DEV * PAGE, HD)
        scores = (
            lax.dot_general(asked, keys, (((1,), (1,)), ((), ())), preferred_element_type=F32)
            * SCALE
        )
        scores = jnp.where(live, scores, NEG_FILL)
        top = jnp.max(scores, axis=1, keepdims=True)
        shift = jnp.where(top > -1e29, jnp.ceil(top * 0.25) * 4.0, NEG_FILL)
        weights = jnp.where(live, jnp.exp(scores - shift), 0.0)
        total = jnp.sum(weights, axis=1, keepdims=True)
        weighted = dot(weights.astype(BF16), values)
        if t >= N_PLANE:
            pair = rs1_pair.at[zs[t - N_PLANE]]
            arrive(pair, t - N_PLANE)
            pair = pair[...].astype(F32)
            pair_out = pair[:, :8].reshape(4 * ROWS, HD)
            pair_stats = pair[:, 8:].reshape(4 * ROWS, HD)
            pair_shift = pair_stats[:, :1]
            pair_total = pair_stats[:, 32:33] + pair_stats[:, 64:65]
            joint = jnp.maximum(shift, pair_shift)
            factor, pair_factor = jnp.exp(shift - joint), jnp.exp(pair_shift - joint)
            total = total * factor + pair_total * pair_factor
            weighted = weighted * factor + pair_out * pair_factor
            shift = joint
        total_high = total.astype(BF16).astype(F32)
        stats = jnp.where(
            lane128 < 32, shift, jnp.where(lane128 < 64, total_high, total - total_high)
        )
        rs1_send[k] = jnp.concatenate(
            [weighted.reshape(16, 8, HD), stats.reshape(16, 8, HD)], axis=1
        ).astype(BF16)

    for t in range(N_PLANE):
        attend_head(t)
        to_other_core(rs1_send.at[kv_heads[t]], rs1_pair.at[zs[t]], t).start()
    slot = z * N_HEAD + head
    for t in range(N_PLANE, N_SEQ):
        attend_head(t)
        for u in range(N_HEAD):
            part = rs1_send.at[kv_heads[t], heads[u]]
            if t > N_PLANE or u:
                remote(part, rs1_recv.at[slot], MERGE, kv_heads[t], heads[u]).start()
            else:
                rs1_recv[slot] = part[...]
    start_bulk(1)

    slot_row, slot_lane = iota((HD, HD), 0), iota((HD, HD), 1)
    wanted_slot = slot_row + lax.rem(head, 2) * SLOTS + seq * SLOTS_DEV
    found = jnp.zeros((HD, HD), jnp.int32)
    for n in range(N_DEV * PG_DEV // HD):
        origin = (n * HD + iota((1, HD), 1)) // PG_DEV
        found = found + jnp.where(all_dests[n : n + 1] == wanted_slot, origin, 0)
    found = jnp.sum(found.astype(F32), axis=1, keepdims=True)
    found = jnp.where(slot_row == slot_lane, found, 0.0)
    chosen[...] = jnp.sum(found, axis=0, keepdims=True).astype(jnp.int32)
    chosen_copy = pltpu.make_async_copy(chosen, chosen_scalars, chosen_sem)
    chosen_copy.start()

    block = lax.rem(me, 4)
    later = block >= 2
    column = queries[:, pl.ds(pl.multiple_of(me // 4 * HD, HD), HD)].astype(F32)
    query = column[:8]
    for n in range(1, 4):
        query = jnp.where(block == n, column[n * 8 : n * 8 + 8], query)
    kv_lane = iota((8, KVH, 2 * HD), 1)
    first_request = lax.rem(block, 2) * 8
    own_fresh = [
        jnp.sum(
            jnp.where(
                kv_lane == me // 16,
                new_kv[u, pl.ds(first_request, 8)].astype(F32),
                0.0,
            ),
            axis=1,
        )
        for u in range(2)
    ]
    fresh_scores = []
    for u in range(2):
        score = jnp.sum(query * own_fresh[u][:, :HD], axis=1, keepdims=True) * SCALE
        fresh_scores.append(score if u == 0 else jnp.where(later, score, NEG_FILL))
    arrive(rs1_recv.at[pl.ds(0, N_DEV // 2 - 1)], MERGE)
    received = rs1_recv[...].astype(F32)
    outs, stats = received[:, :8], received[:, 8:]
    top = jnp.max(stats, axis=0)[:, :1]
    top = jnp.maximum(top, jnp.maximum(fresh_scores[0], fresh_scores[1]))
    factor = jnp.exp(stats[:, :, :1] - top[None])
    weighted = jnp.sum(outs * factor, axis=0)
    totals = jnp.sum(stats * factor, axis=0)
    total = totals[:, 32:33] + totals[:, 64:65]
    for u in range(2):
        weight = jnp.exp(fresh_scores[u] - top)
        total = total + weight
        weighted = weighted + weight.astype(BF16).astype(F32) * own_fresh[u][:, HD:]
    part = (weighted / total).astype(BF16)
    ag1_send[...] = part
    ag1_recv[core, slot] = part

    def gather(part, whole, phase):
        each_of_core(
            lambda to_z, to_head: remote(
                part, whole.at[core, slot], phase, 2 * to_z + core, to_head
            ).start()
        )

    gather(ag1_send, ag1_recv, GATHER_A)
    start_bulk(2)

    select = [
        jnp.where(iota((32, HD), 1) == iota((32, HD), 0) + q * 32, 1.0, 0.0) for q in range(4)
    ]
    router_row = iota((ROWS, EXPERTS), 0)
    wide_router = dot(
        jnp.where(lax.rem(router_row, 16) == iota((ROWS, EXPERTS), 1) + 1, 1.0, 0.0).astype(BF16),
        router[...],
    )
    weight_copies[0].wait()
    def forward(whole, phase, point):
        half = whole.at[core]
        arrive(half.at[pl.ds(0, N_DEV // 2 - 1)], phase)
        to_other_core(half, half, phase + 1).start()
        start_bulk(point)
        arrive(half, phase + 1)

    forward(ag1_recv, GATHER_A, 3)
    for n in range(N_PLANE):
        for c in range(2):
            rows = ag1_recv[c, n * N_HEAD : (n + 1) * N_HEAD].astype(F32).reshape(4, ROWS, HD)
            for g in range(GROUP):
                a = (n * 2 + c) * GROUP + g
                attended[:, a * HD : (a + 1) * HD] = rows[g].astype(BF16)
    middle = hidden[...].astype(F32) + lax.dot_general(
        attended[...], wo[...], (((1,), (1,)), ((), ())), preferred_element_type=F32
    )
    scaled = middle * gain[...].astype(F32)
    lane32 = iota((ROWS, 32), 1)
    sums = lax.dot_general(
        scaled,
        wide_router,
        (((1,), (1,)), ((), ())),
        preferred_element_type=F32,
        precision=HIGHEST,
    )
    square = jnp.sum(middle * middle, axis=1, keepdims=True)
    sums = jnp.where((lane32 == 0) | (lane32 == 16), square, sums)
    sums_high = sums.astype(BF16).astype(F32)
    sums = jnp.where(lane32 < 16, sums_high, sums - sums_high)

    def packed_rows(block, precision=None):
        return sum(
            dot(block[q * 8 : q * 8 + 8], select[q].astype(block.dtype), precision)
            for q in range(4)
        )

    part = jnp.concatenate(
        [packed_rows(scaled.astype(BF16)), packed_rows(sums.astype(BF16))], axis=0
    ).astype(BF16)
    ag2_send[...] = part
    ag2_recv[core, slot] = part
    gather(ag2_send, ag2_recv, GATHER_B)
    start_bulk(4)
    middle_packed = packed_rows(middle, HIGHEST)

    spread_row, spread_col = iota((HD, 512), 0), iota((HD, 512), 1)

    def spread(j):
        wanted = (spread_row // 32) * HD + j * 32 + lax.rem(spread_row, 32)
        return jnp.where(spread_col == wanted, 1.0, 0.0).astype(BF16)

    spreads = [spread(j) for j in range(4)]
    for copy in weight_copies[1:]:
        copy.wait()
    forward(ag2_recv, GATHER_B, 5)
    start_bulk(6)
    received = ag2_recv[...].astype(F32)
    blocks = received[:, :, :8].reshape(32, 4, 8, HD)
    ordered = sum(
        dot(blocks[:, j].reshape(256, HD).astype(BF16), spreads[j]) for j in range(4)
    )
    for n in range(32):
        place = n // 4 % 4 * 8 + n // 16 * 4 + n % 4
        features[:, place * HD : (place + 1) * HD] = jnp.concatenate(
            [ordered[n * 8 : n * 8 + 8, q * HD : (q + 1) * HD] for q in range(4)], axis=0
        ).astype(BF16)
    sums = jnp.sum(jnp.sum(received[:, :, 8:], axis=1), axis=0)
    fold_row, fold_col = iota((HD, HD), 0), iota((HD, HD), 1)
    folded = jnp.concatenate(
        [
            dot(
                sums,
                jnp.where(
                    (fold_row // 32 == q) & (lax.rem(fold_row, 16) == fold_col), 1.0, 0.0
                ),
                HIGHEST,
            )
            for q in range(4)
        ],
        axis=0,
    )
    inverse_rms = lax.rsqrt(folded[:, :1] / D + EPSILON)
    logits = folded * inverse_rms
    diagonal = iota((REQS, REQS), 0) == iota((REQS, REQS), 1)

    def picked(choice):
        rows = [
            jnp.sum(
                jnp.where(diagonal, routes[s, choice : choice + 1, :].astype(F32), 0.0),
                axis=1,
                keepdims=True,
            )
            for s in range(2)
        ]
        return jnp.concatenate(rows, axis=0).astype(jnp.int32)

    first, second = picked(0), picked(1)
    expert_lane = iota((ROWS, HD), 1) - 1
    first_logit = jnp.sum(jnp.where(expert_lane == first, logits, 0.0), axis=1, keepdims=True)
    second_logit = jnp.sum(jnp.where(expert_lane == second, logits, 0.0), axis=1, keepdims=True)
    share = jnp.where(
        first == seq,
        1.0 / (1.0 + jnp.exp(second_logit - first_logit)),
        jnp.where(second == seq, 1.0 / (1.0 + jnp.exp(first_logit - second_logit)), 0.0),
    )
    gate = dot(features[...], wg[...]) * inverse_rms
    upward = dot(features[...], wu[...]) * inverse_rms
    inner = (gate / (1.0 + jnp.exp(-gate)) * upward).astype(BF16)

    collect_row, collect_col = iota((HD, 512), 0), iota((HD, 512), 1)

    def collect(q):
        wanted = (collect_row // 32) * HD + q * 32 + lax.rem(collect_row, 32)
        return jnp.where(collect_col == wanted, 1.0, 0.0).astype(BF16)

    collects = [collect(q) for q in range(4)]
    def produce(parity):
        products = [
            dot(inner, wd[:, pl.ds(pl.multiple_of((2 * n + parity) * 512, 512), 512)]) * share
            for n in range(N_PLANE)
        ]
        return sum(
            dot(
                jnp.concatenate(
                    [
                        product[q * 8 : q * 8 + 8, n * HD : (n + 1) * HD]
                        for product in products
                        for n in range(4)
                    ],
                    axis=0,
                ).astype(BF16),
                collects[q],
            )
            for q in range(4)
        )

    with jax.named_scope("down"):
        parts = produce(other)
        for j in range(4):
            rs2_out[:, j] = parts[:, j * HD : (j + 1) * HD].reshape(16, 8, HD).astype(BF16)
        to_other_core(rs2_out, rs2_pair, PAIR_SUMS).start()
        parts = produce(core)
    arrive(rs2_pair, PAIR_SUMS)
    for j in range(4):
        part = parts[:, j * HD : (j + 1) * HD].reshape(16, 8, HD)
        rs2_send[:, j] = (part + rs2_pair[:, j].astype(F32)).astype(BF16)
    rs2_recv[slot] = rs2_send[slot // 4, lax.rem(slot, 4)]

    def send_sums(to_z, to_head):
        part = rs2_send.at[to_z * 4 + to_head // 4, lax.rem(to_head, 4)]
        remote(part, rs2_recv.at[slot], SUMS, 2 * to_z + core, to_head).start()

    each_of_core(send_sums)
    start_bulk(7)
    arrive(rs2_recv.at[pl.ds(0, N_DEV // 2 - 1)], SUMS)
    block = middle_packed + jnp.sum(rs2_recv[...].astype(F32), axis=0)
    for s in range(2):
        mixed[s] = jnp.concatenate(
            [block[:, q * 32 : (q + 1) * 32] for q in (2 * s, 2 * s + 1)], axis=0
        ).astype(BF16)
    chosen_copy.wait()

    most = N_DEV // 2 - 1
    for t in range(N_PLANE):
        received_all(rs1_pair.at[t], t).wait_send()
    for rest, phase in (
        (rs1_recv.at[pl.ds(0, most)], MERGE),
        (ag1_recv.at[0, pl.ds(0, most)], GATHER_A),
        (ag1_recv.at[0], FORWARD_A),
        (ag2_recv.at[0, pl.ds(0, most)], GATHER_B),
        (ag2_recv.at[0], FORWARD_B),
        (rs2_pair, PAIR_SUMS),
        (rs2_recv.at[pl.ds(0, most)], SUMS),
    ):
        received_all(rest, phase).wait_send()
    arrive(arrived.at[pl.ds(0, N_DEV - 1)], BULK)
    finish_pages()
    with jax.named_scope("place"):

        def place(n, carry):
            for j in range(8):
                origin = jnp.clip(chosen_scalars[0, n * 8 + j], 0, N_DEV - 1)
                pool[n * 8 + j] = arrived[origin]
            return carry

        lax.fori_loop(0, SLOTS_DEV // 8, place, 0)


def finish_kernel(pool, mixed, pool_out, mixed_out, sem):
    parts = [
        pltpu.make_async_copy(
            pool.at[pl.ds(n * 16, 16)], pool_out.at[pl.ds(n * 16, 16)], sem.at[n]
        )
        for n in range(6)
    ]
    parts.append(pltpu.make_async_copy(mixed, mixed_out, sem.at[6]))
    for part in parts:
        part.start()
    for part in parts:
        part.wait()


def body(
    lengths,
    page_owner,
    page_index,
    page_dest,
    src_cache,
    queries,
    new_kv,
    hidden_in,
    out_weight,
    norm_gain,
    router,
    routes,
    w_gate,
    w_up,
    w_down,
):
    vmem = pl.BlockSpec(memory_space=pltpu.VMEM)
    hbm = pl.BlockSpec(memory_space=pltpu.HBM)
    page_pool, mixed = pl.pallas_call(
        decode_kernel,
        out_shape=(
            pltpu.VMEM((SLOTS_DEV, PAGE, 2 * HD), BF16),
            pltpu.VMEM((2, REQS, 32), BF16),
        ),
        in_specs=[hbm] * 16,
        out_specs=(vmem, vmem),
        scratch_shapes=[
            pltpu.SMEM((REQS,), jnp.int32),
            pltpu.SMEM((N_DEV * PG_DEV,), jnp.int32),
            pltpu.SMEM((N_DEV * PG_DEV,), jnp.int32),
            pltpu.SMEM((N_DEV * PG_DEV,), jnp.int32),
            pltpu.VMEM((N_DEV * PG_DEV // HD, HD), jnp.int32),
            pltpu.VMEM((2, REQS, KVH, 2 * HD), BF16),
            pltpu.VMEM((ROWS, 32), BF16),
            pltpu.VMEM((1, 32), BF16),
            pltpu.VMEM((EXPERTS, 32), BF16),
            pltpu.VMEM((2, 2, REQS), jnp.int32),
            pltpu.VMEM((1, HD), jnp.int32),
            pltpu.SMEM((1, HD), jnp.int32),
            pltpu.VMEM((N_DEV, PAGE, 2 * HD), BF16),
            pltpu.VMEM((PG_DEV, KVH, PAGE, 2 * HD), BF16),
            pltpu.VMEM((2 * N_SEQ, KVH, PAGE, 2 * HD), BF16),
            pltpu.VMEM((ROWS, D), BF16),
            pltpu.VMEM((32, D), BF16),
            pltpu.VMEM((D, FF_DEV), BF16),
            pltpu.VMEM((D, FF_DEV), BF16),
            pltpu.VMEM((FF_DEV, D), BF16),
            pltpu.VMEM((KVH, 16, 16, HD), BF16),
            pltpu.VMEM((N_PLANE, 16, 16, HD), BF16),
            pltpu.VMEM((N_DEV // 2, 16, HD), BF16),
            pltpu.VMEM((8, HD), BF16),
            pltpu.VMEM((2, N_DEV // 2, 8, HD), BF16),
            pltpu.VMEM((ROWS, D), BF16),
            pltpu.VMEM((16, HD), BF16),
            pltpu.VMEM((2, N_DEV // 2, 16, HD), BF16),
            pltpu.VMEM((ROWS, D), BF16),
            pltpu.VMEM((16, 4, 8, HD), BF16),
            pltpu.VMEM((16, 4, 8, HD), BF16),
            pltpu.VMEM((16, 4, 8, HD), BF16),
            pltpu.VMEM((N_DEV // 2, 8, HD), BF16),
            pltpu.SemaphoreType.DMA((10,)),
            pltpu.SemaphoreType.DMA,
            pltpu.SemaphoreType.DMA((N_SEQ,)),
            pltpu.SemaphoreType.DMA,
            pltpu.SemaphoreType.DMA((4,)),
            pltpu.SemaphoreType.DMA((PACED + len(BULK_STARTS),)),
            pltpu.SemaphoreType.DMA((12,)),
            pltpu.SemaphoreType.DMA((12,)),
        ],
        compiler_params=pltpu.CompilerParams(
            collective_id=0, has_side_effects=True, vmem_limit_bytes=60 * 1024 * 1024
        ),
        name="decode",
    )(
        lengths,
        page_owner,
        page_index,
        page_dest,
        page_dest.reshape(N_DEV * PG_DEV // HD, HD),
        src_cache,
        queries.reshape(ROWS, HQ * HD),
        new_kv,
        hidden_in.reshape(ROWS, 32),
        out_weight.T,
        norm_gain.reshape(1, 32),
        router.T,
        routes.transpose(0, 2, 1),
        w_gate[0],
        w_up[0],
        w_down[0],
    )
    page_pool, mixed = pl.pallas_call(
        finish_kernel,
        out_shape=(
            jax.ShapeDtypeStruct((SLOTS_DEV, PAGE, 2 * HD), BF16),
            jax.ShapeDtypeStruct((2, REQS, 32), BF16),
        ),
        in_specs=[vmem, vmem],
        out_specs=(hbm, hbm),
        scratch_shapes=[pltpu.SemaphoreType.DMA((7,))],
        compiler_params=pltpu.CompilerParams(vmem_limit_bytes=1024 * 1024),
        name="finish",
    )(
        pltpu.with_memory_space_constraint(page_pool, pltpu.VMEM),
        pltpu.with_memory_space_constraint(mixed, pltpu.VMEM),
    )
    return (page_pool[None], mixed)


def solution(mesh):
    in_specs = (
        P(),
        P(),
        P(),
        P(),
        P(SEQ_HEAD, None, None, None),
        P(),
        P(),
        P(None, None, SEQ_HEAD),
        P(None, SEQ_HEAD),
        P(SEQ_HEAD),
        P(SEQ_HEAD, None),
        P(),
        P("seq", None, "head"),
        P("seq", None, "head"),
        P("seq", "head", None),
    )
    out_specs = (P("head", "seq", None, None), P(None, None, SEQ_HEAD))
    return jax.shard_map(body, mesh=mesh, in_specs=in_specs, out_specs=out_specs, check_vma=False)
```

```python
import functools

import jax
import jax.numpy as jnp
from jax import lax
from jax.experimental import pallas as pl
from jax.experimental.pallas import tpu as pltpu
from jax.sharding import PartitionSpec as P

D = 4096
HQ = 32
KVH = 8
GROUP = HQ // KVH
HD = 128
EXPERTS = 8
PAGE = 64
REQS = 16
ROWS = 32
FF_DEV = 512
PG_DEV = 12
SLOTS = 768
SLOTS_DEV = 96
N_SEQ = 8
N_HEAD = 16
N_DEV = N_SEQ * N_HEAD
NEG_FILL = -1e30
EPSILON = 1e-05
HIGHEST = lax.Precision.HIGHEST
SCALE = HD ** (-0.5)
SEQ_HEAD = ("seq", "head")
BF16 = jnp.bfloat16
F32 = jnp.float32
N_PLANE = 4
PACED = 4
BULK_STARTS = ((16, 0), (12, 1), (12, 1), (5, 0), (12, 1), (4, 0), (28, 0), (38, 0))
MERGE, GATHER_A, FORWARD_A, GATHER_B, FORWARD_B, PAIR_SUMS, SUMS, BULK = range(4, 12)


def farthest_first(offsets):
    return sorted(offsets, key=lambda o: -sum(min(d, 4 - d) for d in o))


def balanced_order():
    left = [(n // 32, n // 16 % 2, n // 4 % 4, n % 4) for n in range(1, N_DEV)]
    loads, order = [0.0] * 6, []

    def added(offset):
        new = list(loads)
        for axis, d in enumerate((offset[2], offset[3], offset[0])):
            for way, amount in enumerate(((0, 1, 1, 0), (0, 0, 1, 1))):
                new[2 * axis + way] += amount[d]
        return new

    def spread(offset):
        new = added(offset)
        mean = sum(new) / 6
        return sum((n - mean) ** 2 for n in new), -sum(new)

    while left:
        best = min(left, key=spread)
        loads = added(best)
        left.remove(best)
        order.append(best)
    return order


PAGE_ORDER = balanced_order()
PLANE_OFFSETS = farthest_first([(n // 16, n // 4 % 4, n % 4) for n in range(1, 64)])


def iota(shape, dim):
    return lax.broadcasted_iota(jnp.int32, shape, dim)


def dot(a, b, precision=None):
    return jnp.dot(a, b, preferred_element_type=F32, precision=precision)


def decode_kernel(
    lengths_hbm,
    page_owner_hbm,
    page_index_hbm,
    page_dest_hbm,
    all_dests_hbm,
    src_hbm,
    queries_hbm,
    new_kv_hbm,
    hidden_hbm,
    wo_hbm,
    gain_hbm,
    router_hbm,
    routes_hbm,
    wg_hbm,
    wu_hbm,
    wd_hbm,
    pool,
    mixed,
    lengths,
    page_owner,
    page_index,
    page_dest,
    all_dests,
    new_kv,
    hidden,
    gain,
    router,
    routes,
    chosen,
    chosen_scalars,
    arrived,
    src,
    packed,
    queries,
    wo,
    wg,
    wu,
    wd,
    rs1_send,
    rs1_pair,
    rs1_recv,
    ag1_send,
    ag1_recv,
    attended,
    ag2_send,
    ag2_recv,
    features,
    all_router,
    all_gain,
    rs2_out,
    rs2_pair,
    rs2_send,
    rs2_recv,
    small_sem,
    chosen_sem,
    src_sem,
    query_sem,
    weight_sem,
    page_sem,
    send_sem,
    recv_sem,
):
    seq = lax.axis_index("seq")
    head = lax.axis_index("head")
    me = seq * N_HEAD + head
    heads = [lax.rem(head + u, N_HEAD) for u in range(N_HEAD)]
    z, core, x, y = seq // 2, lax.rem(seq, 2), head // 4, lax.rem(head, 4)
    zs = [lax.rem(z + t, 4) for t in range(4)]
    cores = [lax.rem(core + t, 2) for t in range(2)]
    xs = [lax.rem(x + t, 4) for t in range(4)]
    ys = [lax.rem(y + t, 4) for t in range(4)]
    other = 1 - core
    kv_heads = [2 * zs[t] + other for t in range(N_PLANE)] + [2 * zs[t] + core for t in range(N_PLANE)]

    def page_copy(t):
        return pltpu.make_async_copy(
            src_hbm.at[:, kv_heads[t]], src.at[:, kv_heads[t]], src_sem.at[t]
        )

    query_copy = pltpu.make_async_copy(queries_hbm, queries, query_sem)
    weight_copies = [
        pltpu.make_async_copy(a, b, weight_sem.at[n])
        for n, (a, b) in enumerate(((wo_hbm, wo), (wg_hbm, wg), (wu_hbm, wu), (wd_hbm, wd)))
    ]
    barrier = pltpu.get_barrier_semaphore()

    @jax.named_scope("greet")
    def each_peer(act):
        for dz, dx, dy in PLANE_OFFSETS:
            for to_core in (other, core):
                act(2 * zs[dz] + to_core, 4 * xs[dx] + ys[dy])
        act(2 * z + other, head)

    @jax.named_scope("each_plane")
    def each_of_core(act):
        for dz, dx, dy in PLANE_OFFSETS:
            act(zs[dz], 4 * xs[dx] + ys[dy])

    def greet(to_seq, to_head):
        pl.semaphore_signal(
            barrier,
            inc=1,
            device_id=(to_seq, to_head),
            device_id_type=pl.DeviceIdType.MESH,
        )

    small_copies = [
        pltpu.make_async_copy(a, b, small_sem.at[n])
        for n, (a, b) in enumerate(
            (
                (lengths_hbm, lengths),
                (page_owner_hbm, page_owner),
                (page_index_hbm, page_index),
                (page_dest_hbm, page_dest),
                (all_dests_hbm, all_dests),
                (new_kv_hbm, new_kv),
                (hidden_hbm, hidden),
                (gain_hbm, gain),
                (router_hbm, router),
                (routes_hbm, routes),
            )
        )
    ]
    for t in range(N_SEQ):
        page_copy(t).start()
    for copy in small_copies:
        copy.start()
    query_copy.start()
    each_peer(greet)
    with jax.named_scope("small"):
        for copy in small_copies:
            copy.wait()

    def remote(source, target, phase, to_seq, to_head):
        return pltpu.make_async_remote_copy(
            src_ref=source,
            dst_ref=target,
            send_sem=send_sem.at[phase],
            recv_sem=recv_sem.at[phase],
            device_id=(to_seq, to_head),
            device_id_type=pl.DeviceIdType.MESH,
        )

    def to_other_core(source, target, phase):
        return remote(source, target, phase, 2 * z + other, head)

    def received_all(rest, phase):
        return remote(rest, rest, phase, 2 * z + other, head)

    def arrive(rest, phase):
        with jax.named_scope(f"arrive{phase}"):
            received_all(rest, phase).wait_recv()

    lane = iota((1, PG_DEV * PAGE), 1)
    token_owner = jnp.full((1, PG_DEV * PAGE), REQS, jnp.int32)
    for p in range(PG_DEV):
        owner = page_owner[me * PG_DEV + p]
        limit = lengths[jnp.minimum(owner, REQS - 1)] - page_index[me * PG_DEV + p] * PAGE
        inside = (lane >= p * PAGE) & (lane < p * PAGE + jnp.minimum(limit, PAGE))
        token_owner = jnp.where(inside, owner, token_owner)

    @jax.named_scope("pack")
    def pack_pages():
        groups = []
        for p in range(PG_DEV):
            dest = page_dest[me * PG_DEV + p]
            upper = jnp.where(dest >= SLOTS, 1, 0)
            within = dest - upper * SLOTS
            target = jnp.int32(0)
            for n in range(1, N_SEQ):
                target = target + jnp.where(within >= n * SLOTS_DEV, 2, 0)
            groups.append(target + upper)

        def one(group, carry):
            page = jnp.int32(0)
            for p in range(PG_DEV):
                page = jnp.where(groups[p] == group, p, page)
            for k in range(KVH):
                packed[group, k] = src[page, k]
            return carry

        lax.fori_loop(0, 2 * N_SEQ, one, 0)

    started, paced = [0], []

    def page_send(i, sem):
        dz, dc, dx, dy = PAGE_ORDER[i]
        to_seq = zs[dz] * 2 + cores[dc]
        to_head = xs[dx] * 4 + ys[dy]
        part = packed.at[to_seq * 2 + lax.rem(to_head, 2), to_head // 2]
        return pltpu.make_async_remote_copy(
            src_ref=part,
            dst_ref=arrived.at[me],
            send_sem=page_sem.at[sem],
            recv_sem=recv_sem.at[BULK],
            device_id=(to_seq, to_head),
            device_id_type=pl.DeviceIdType.MESH,
        )

    @jax.named_scope("bulk")
    def start_bulk(point, begin=0, end=None):
        count, window = BULK_STARTS[point]
        count = (count if end is None else end) - begin
        for i in range(started[0], started[0] + count):
            sem = PACED + point
            if window:
                sem = len(paced) % PACED
                if len(paced) >= PACED:
                    page_send(*paced[-PACED]).wait_send()
                paced.append((i, sem))
            page_send(i, sem).start()
        started[0] += count

    def finish_pages():
        for i, sem in paced[-PACED:]:
            page_send(i, sem).wait_send()
        for point, (count, window) in enumerate(BULK_STARTS):
            if not window:
                rest = arrived.at[pl.ds(0, count)]
                pltpu.make_async_remote_copy(
                    src_ref=rest,
                    dst_ref=rest,
                    send_sem=page_sem.at[PACED + point],
                    recv_sem=recv_sem.at[BULK],
                    device_id=(2 * z + other, head),
                    device_id_type=pl.DeviceIdType.MESH,
                ).wait_send()

    row_request = lax.rem(iota((4 * ROWS, 1), 0), REQS)
    live = token_owner == row_request
    lane128 = iota((4 * ROWS, HD), 1)
    with jax.named_scope("pages"):
        for t in range(N_SEQ):
            page_copy(t).wait()
    query_copy.wait()
    for copy in weight_copies:
        copy.start()
    pack_pages()
    with jax.named_scope("greeted"):
        pl.semaphore_wait(barrier, N_DEV - 1)
    arrived[me] = packed[seq * 2 + lax.rem(head, 2), head // 2]
    start_bulk(0)

    tile_row, tile_lane = iota((8, HD), 0), iota((8, HD), 1)

    def to_lanes(block, first):
        shifted = jnp.where(iota((32, HD), 1) == iota((32, HD), 0) + first, 1.0, 0.0)
        return dot(block, shifted.astype(BF16))

    own_gain = jnp.where(iota((8, 32), 0) == 0, gain[...].astype(F32), 0.0).astype(BF16)
    own_extra = to_lanes(own_gain, 32) + to_lanes(router[...], 64)
    extras = [own_extra]

    def chip_extra():
        pair = rs1_pair[zs[0], 0].astype(F32)[8:]
        gains = jnp.where(
            (tile_lane >= 32) & (tile_lane < 64) & (tile_row == 1), pltpu.roll(pair, 1, 0), 0.0
        )
        routers = jnp.where(tile_lane >= 96, pltpu.roll(pair, 32, 1), 0.0)
        return own_extra + gains + routers

    @jax.named_scope("attend")
    def attend_head(t):
        k = kv_heads[t]
        asked = jnp.concatenate(
            [
                queries[:, pl.ds(pl.multiple_of((k * GROUP + g) * HD, HD), HD)]
                for g in range(GROUP)
            ],
            axis=0,
        )
        keys = src[:, k, :, :HD].reshape(PG_DEV * PAGE, HD)
        values = src[:, k, :, HD:].reshape(PG_DEV * PAGE, HD)
        scores = (
            lax.dot_general(asked, keys, (((1,), (1,)), ((), ())), preferred_element_type=F32)
            * SCALE
        )
        scores = jnp.where(live, scores, NEG_FILL)
        top = jnp.max(scores, axis=1, keepdims=True)
        shift = jnp.where(top > -1e29, jnp.ceil(top * 0.25) * 4.0, NEG_FILL)
        weights = jnp.where(live, jnp.exp(scores - shift), 0.0)
        total = jnp.sum(weights, axis=1, keepdims=True)
        weighted = dot(weights.astype(BF16), values)
        if t >= N_PLANE:
            pair = rs1_pair.at[zs[t - N_PLANE]]
            arrive(pair, t - N_PLANE)
            if t == N_PLANE:
                extras[0] = chip_extra()
            pair = pair[...].astype(F32)
            pair_out = pair[:, :8].reshape(4 * ROWS, HD)
            pair_stats = pair[:, 8:].reshape(4 * ROWS, HD)
            pair_shift = pair_stats[:, :1]
            pair_total = pair_stats[:, 8:9] + pair_stats[:, 16:17]
            joint = jnp.maximum(shift, pair_shift)
            factor, pair_factor = jnp.exp(shift - joint), jnp.exp(pair_shift - joint)
            total = total * factor + pair_total * pair_factor
            weighted = weighted * factor + pair_out * pair_factor
            shift = joint
        total_high = total.astype(BF16).astype(F32)
        stats = jnp.where(
            lane128 < 8, shift, jnp.where(lane128 < 16, total_high, total - total_high)
        )
        extra = jnp.broadcast_to(extras[0][None], (16, 8, HD)).reshape(4 * ROWS, HD)
        stats = jnp.where(lane128 < 32, stats, extra)
        rs1_send[k] = jnp.concatenate(
            [weighted.reshape(16, 8, HD), stats.reshape(16, 8, HD)], axis=1
        ).astype(BF16)

    for t in range(N_PLANE):
        attend_head(t)
        to_other_core(rs1_send.at[kv_heads[t]], rs1_pair.at[zs[t]], t).start()
    slot = z * N_HEAD + head
    for t in range(N_PLANE, N_SEQ):
        attend_head(t)
        for u in range(N_HEAD):
            part = rs1_send.at[kv_heads[t], heads[u]]
            if t > N_PLANE or u:
                remote(part, rs1_recv.at[slot], MERGE, kv_heads[t], heads[u]).start()
            else:
                rs1_recv[slot] = part[...]
    start_bulk(1, 0, PACED)

    slot_row, slot_lane = iota((HD, HD), 0), iota((HD, HD), 1)
    wanted_slot = slot_row + lax.rem(head, 2) * SLOTS + seq * SLOTS_DEV
    found = jnp.zeros((HD, HD), jnp.int32)
    for n in range(N_DEV * PG_DEV // HD):
        origin = (n * HD + iota((1, HD), 1)) // PG_DEV
        found = found + jnp.where(all_dests[n : n + 1] == wanted_slot, origin, 0)
    found = jnp.sum(found.astype(F32), axis=1, keepdims=True)
    found = jnp.where(slot_row == slot_lane, found, 0.0)
    chosen[...] = jnp.sum(found, axis=0, keepdims=True).astype(jnp.int32)
    chosen_copy = pltpu.make_async_copy(chosen, chosen_scalars, chosen_sem)
    chosen_copy.start()

    block = lax.rem(me, 4)
    later = block >= 2
    column = queries[:, pl.ds(pl.multiple_of(me // 4 * HD, HD), HD)].astype(F32)
    query = column[:8]
    for n in range(1, 4):
        query = jnp.where(block == n, column[n * 8 : n * 8 + 8], query)
    kv_lane = iota((8, KVH, 2 * HD), 1)
    first_request = lax.rem(block, 2) * 8
    own_fresh = [
        jnp.sum(
            jnp.where(
                kv_lane == me // 16,
                new_kv[u, pl.ds(first_request, 8)].astype(F32),
                0.0,
            ),
            axis=1,
        )
        for u in range(2)
    ]
    fresh_scores = []
    for u in range(2):
        score = jnp.sum(query * own_fresh[u][:, :HD], axis=1, keepdims=True) * SCALE
        fresh_scores.append(score if u == 0 else jnp.where(later, score, NEG_FILL))
    start_bulk(1, PACED)
    arrive(rs1_recv.at[pl.ds(0, N_DEV // 2 - 1)], MERGE)
    received = rs1_recv[...].astype(F32)
    outs, stats = received[:, :8], received[:, 8:]
    top = jnp.max(stats, axis=0)[:, :1]
    top = jnp.maximum(top, jnp.maximum(fresh_scores[0], fresh_scores[1]))
    factor = jnp.exp(stats[:, :, :1] - top[None])
    weighted = jnp.sum(outs * factor, axis=0)
    totals = jnp.sum(stats * factor, axis=0)
    total = totals[:, 8:9] + totals[:, 16:17]
    for u in range(2):
        weight = jnp.exp(fresh_scores[u] - top)
        total = total + weight
        weighted = weighted + weight.astype(BF16).astype(F32) * own_fresh[u][:, HD:]
    part = (weighted / total).astype(BF16)
    ag1_send[...] = part
    ag1_recv[core, slot] = part

    def gather(part, whole, phase):
        each_of_core(
            lambda to_z, to_head: remote(
                part, whole.at[core, slot], phase, 2 * to_z + core, to_head
            ).start()
        )

    gather(ag1_send, ag1_recv, GATHER_A)
    start_bulk(2, 0, PACED)

    select = [
        jnp.where(iota((32, HD), 1) == iota((32, HD), 0) + q * 32, 1.0, 0.0) for q in range(4)
    ]
    extra_blocks = stats.reshape(16, 4, 8, HD)
    move_row, move_lane = iota((HD, HD), 0), iota((HD, HD), 1)

    def in_order(first):
        return sum(
            dot(
                extra_blocks[:, j].reshape(HD, HD).astype(BF16),
                jnp.where(
                    (move_row - first == move_lane - j * 32)
                    & (move_lane >= j * 32)
                    & (move_lane < j * 32 + 32),
                    1.0,
                    0.0,
                ).astype(BF16),
            )
            for j in range(4)
        )

    gains, own_routers, other_routers = in_order(32), in_order(64), in_order(96)
    first_core = core == 0
    for n in range(N_PLANE * 4):
        rows = slice(n * 8, n * 8 + 8)
        routers = (
            jnp.where(first_core, own_routers[rows], other_routers[rows]),
            jnp.where(first_core, other_routers[rows], own_routers[rows]),
        )
        pair_gains = gains[rows]
        both = (
            jnp.where(first_core, pair_gains[0:1], pair_gains[1:2]),
            jnp.where(first_core, pair_gains[1:2], pair_gains[0:1]),
        )
        for c in range(2):
            place = n // 4 * 8 + c * 4 + n % 4
            all_router[:, place * HD : (place + 1) * HD] = routers[c].astype(BF16)
            all_gain[:, place * HD : (place + 1) * HD] = 1.0 / both[c]
    weight_copies[0].wait()
    def forward(whole, phase, point):
        half = whole.at[core]
        arrive(half.at[pl.ds(0, N_DEV // 2 - 1)], phase)
        to_other_core(half, half, phase + 1).start()
        start_bulk(point)
        arrive(half, phase + 1)

    start_bulk(2, PACED)
    forward(ag1_recv, GATHER_A, 3)
    for n in range(N_PLANE):
        for c in range(2):
            rows = ag1_recv[c, n * N_HEAD : (n + 1) * N_HEAD].astype(F32).reshape(4, ROWS, HD)
            for g in range(GROUP):
                a = (n * 2 + c) * GROUP + g
                attended[:, a * HD : (a + 1) * HD] = rows[g].astype(BF16)
    middle = hidden[...].astype(F32) + lax.dot_general(
        attended[...], wo[...], (((1,), (1,)), ((), ())), preferred_element_type=F32
    )
    scaled = middle * gain[...].astype(F32)

    def packed_rows(block, precision=None):
        return sum(
            dot(block[q * 8 : q * 8 + 8], select[q].astype(block.dtype), precision)
            for q in range(4)
        )

    part = packed_rows(scaled.astype(BF16)).astype(BF16)
    ag2_send[...] = part
    ag2_recv[core, slot] = part
    gather(ag2_send, ag2_recv, GATHER_B)
    start_bulk(4, 0, PACED)
    middle_packed = packed_rows(middle, HIGHEST)

    spread_row, spread_col = iota((HD, 512), 0), iota((HD, 512), 1)

    def spread(j):
        wanted = (spread_row // 32) * HD + j * 32 + lax.rem(spread_row, 32)
        return jnp.where(spread_col == wanted, 1.0, 0.0).astype(BF16)

    spreads = [spread(j) for j in range(4)]
    for copy in weight_copies[1:]:
        copy.wait()
    start_bulk(4, PACED)
    forward(ag2_recv, GATHER_B, 5)
    start_bulk(6)
    received = ag2_recv[...].astype(F32)
    blocks = received.reshape(32, 4, 8, HD)
    ordered = sum(
        dot(blocks[:, j].reshape(256, HD).astype(BF16), spreads[j]) for j in range(4)
    )
    for n in range(32):
        place = n // 4 % 4 * 8 + n // 16 * 4 + n % 4
        features[:, place * HD : (place + 1) * HD] = jnp.concatenate(
            [ordered[n * 8 : n * 8 + 8, q * HD : (q + 1) * HD] for q in range(4)], axis=0
        ).astype(BF16)
    whole = features[...]
    unscaled = whole.astype(F32) * all_gain[...]
    squares = jnp.sum(unscaled * unscaled, axis=1, keepdims=True)
    inverse_rms = lax.rsqrt(squares / D + EPSILON)
    logits = inverse_rms * lax.dot_general(
        whole, all_router[...], (((1,), (1,)), ((), ())), preferred_element_type=F32
    )
    diagonal = iota((REQS, REQS), 0) == iota((REQS, REQS), 1)

    def picked(choice):
        rows = [
            jnp.sum(
                jnp.where(diagonal, routes[s, choice : choice + 1, :].astype(F32), 0.0),
                axis=1,
                keepdims=True,
            )
            for s in range(2)
        ]
        return jnp.concatenate(rows, axis=0).astype(jnp.int32)

    first, second = picked(0), picked(1)
    expert_lane = iota((ROWS, EXPERTS), 1)
    first_logit = jnp.sum(jnp.where(expert_lane == first, logits, 0.0), axis=1, keepdims=True)
    second_logit = jnp.sum(jnp.where(expert_lane == second, logits, 0.0), axis=1, keepdims=True)
    share = jnp.where(
        first == seq,
        1.0 / (1.0 + jnp.exp(second_logit - first_logit)),
        jnp.where(second == seq, 1.0 / (1.0 + jnp.exp(first_logit - second_logit)), 0.0),
    )
    gate = dot(features[...], wg[...]) * inverse_rms
    upward = dot(features[...], wu[...]) * inverse_rms
    inner = (gate / (1.0 + jnp.exp(-gate)) * upward).astype(BF16)

    collect_row, collect_col = iota((HD, 512), 0), iota((HD, 512), 1)

    def collect(q):
        wanted = (collect_row // 32) * HD + q * 32 + lax.rem(collect_row, 32)
        return jnp.where(collect_col == wanted, 1.0, 0.0).astype(BF16)

    collects = [collect(q) for q in range(4)]
    def produce(parity):
        products = [
            dot(inner, wd[:, pl.ds(pl.multiple_of((2 * n + parity) * 512, 512), 512)]) * share
            for n in range(N_PLANE)
        ]
        return sum(
            dot(
                jnp.concatenate(
                    [
                        product[q * 8 : q * 8 + 8, n * HD : (n + 1) * HD]
                        for product in products
                        for n in range(4)
                    ],
                    axis=0,
                ).astype(BF16),
                collects[q],
            )
            for q in range(4)
        )

    with jax.named_scope("down"):
        parts = produce(other)
        for j in range(4):
            rs2_out[:, j] = parts[:, j * HD : (j + 1) * HD].reshape(16, 8, HD).astype(BF16)
        to_other_core(rs2_out, rs2_pair, PAIR_SUMS).start()
        parts = produce(core)
    arrive(rs2_pair, PAIR_SUMS)
    for j in range(4):
        part = parts[:, j * HD : (j + 1) * HD].reshape(16, 8, HD)
        rs2_send[:, j] = (part + rs2_pair[:, j].astype(F32)).astype(BF16)
    rs2_recv[slot] = rs2_send[slot // 4, lax.rem(slot, 4)]

    def send_sums(to_z, to_head):
        part = rs2_send.at[to_z * 4 + to_head // 4, lax.rem(to_head, 4)]
        remote(part, rs2_recv.at[slot], SUMS, 2 * to_z + core, to_head).start()

    each_of_core(send_sums)
    start_bulk(7)
    arrive(rs2_recv.at[pl.ds(0, N_DEV // 2 - 1)], SUMS)
    block = middle_packed + jnp.sum(rs2_recv[...].astype(F32), axis=0)
    for s in range(2):
        mixed[s] = jnp.concatenate(
            [block[:, q * 32 : (q + 1) * 32] for q in (2 * s, 2 * s + 1)], axis=0
        ).astype(BF16)
    chosen_copy.wait()

    most = N_DEV // 2 - 1
    for t in range(N_PLANE):
        received_all(rs1_pair.at[t], t).wait_send()
    for rest, phase in (
        (rs1_recv.at[pl.ds(0, most)], MERGE),
        (ag1_recv.at[0, pl.ds(0, most)], GATHER_A),
        (ag1_recv.at[0], FORWARD_A),
        (ag2_recv.at[0, pl.ds(0, most)], GATHER_B),
        (ag2_recv.at[0], FORWARD_B),
        (rs2_pair, PAIR_SUMS),
        (rs2_recv.at[pl.ds(0, most)], SUMS),
    ):
        received_all(rest, phase).wait_send()
    arrive(arrived.at[pl.ds(0, N_DEV - 1)], BULK)
    finish_pages()
    with jax.named_scope("place"):

        def place(n, carry):
            for j in range(8):
                origin = jnp.clip(chosen_scalars[0, n * 8 + j], 0, N_DEV - 1)
                pool[n * 8 + j] = arrived[origin]
            return carry

        lax.fori_loop(0, SLOTS_DEV // 8, place, 0)


def finish_kernel(pool, mixed, pool_out, mixed_out, sem):
    parts = [
        pltpu.make_async_copy(
            pool.at[pl.ds(n * 16, 16)], pool_out.at[pl.ds(n * 16, 16)], sem.at[n]
        )
        for n in range(6)
    ]
    parts.append(pltpu.make_async_copy(mixed, mixed_out, sem.at[6]))
    for part in parts:
        part.start()
    for part in parts:
        part.wait()


def body(
    lengths,
    page_owner,
    page_index,
    page_dest,
    src_cache,
    queries,
    new_kv,
    hidden_in,
    out_weight,
    norm_gain,
    router,
    routes,
    w_gate,
    w_up,
    w_down,
):
    vmem = pl.BlockSpec(memory_space=pltpu.VMEM)
    hbm = pl.BlockSpec(memory_space=pltpu.HBM)
    page_pool, mixed = pl.pallas_call(
        decode_kernel,
        out_shape=(
            pltpu.VMEM((SLOTS_DEV, PAGE, 2 * HD), BF16),
            pltpu.VMEM((2, REQS, 32), BF16),
        ),
        in_specs=[hbm] * 16,
        out_specs=(vmem, vmem),
        scratch_shapes=[
            pltpu.SMEM((REQS,), jnp.int32),
            pltpu.SMEM((N_DEV * PG_DEV,), jnp.int32),
            pltpu.SMEM((N_DEV * PG_DEV,), jnp.int32),
            pltpu.SMEM((N_DEV * PG_DEV,), jnp.int32),
            pltpu.VMEM((N_DEV * PG_DEV // HD, HD), jnp.int32),
            pltpu.VMEM((2, REQS, KVH, 2 * HD), BF16),
            pltpu.VMEM((ROWS, 32), BF16),
            pltpu.VMEM((1, 32), BF16),
            pltpu.VMEM((EXPERTS, 32), BF16),
            pltpu.VMEM((2, 2, REQS), jnp.int32),
            pltpu.VMEM((1, HD), jnp.int32),
            pltpu.SMEM((1, HD), jnp.int32),
            pltpu.VMEM((N_DEV, PAGE, 2 * HD), BF16),
            pltpu.VMEM((PG_DEV, KVH, PAGE, 2 * HD), BF16),
            pltpu.VMEM((2 * N_SEQ, KVH, PAGE, 2 * HD), BF16),
            pltpu.VMEM((ROWS, D), BF16),
            pltpu.VMEM((32, D), BF16),
            pltpu.VMEM((D, FF_DEV), BF16),
            pltpu.VMEM((D, FF_DEV), BF16),
            pltpu.VMEM((FF_DEV, D), BF16),
            pltpu.VMEM((KVH, 16, 16, HD), BF16),
            pltpu.VMEM((N_PLANE, 16, 16, HD), BF16),
            pltpu.VMEM((N_DEV // 2, 16, HD), BF16),
            pltpu.VMEM((8, HD), BF16),
            pltpu.VMEM((2, N_DEV // 2, 8, HD), BF16),
            pltpu.VMEM((ROWS, D), BF16),
            pltpu.VMEM((8, HD), BF16),
            pltpu.VMEM((2, N_DEV // 2, 8, HD), BF16),
            pltpu.VMEM((ROWS, D), BF16),
            pltpu.VMEM((EXPERTS, D), BF16),
            pltpu.VMEM((1, D), F32),
            pltpu.VMEM((16, 4, 8, HD), BF16),
            pltpu.VMEM((16, 4, 8, HD), BF16),
            pltpu.VMEM((16, 4, 8, HD), BF16),
            pltpu.VMEM((N_DEV // 2, 8, HD), BF16),
            pltpu.SemaphoreType.DMA((10,)),
            pltpu.SemaphoreType.DMA,
            pltpu.SemaphoreType.DMA((N_SEQ,)),
            pltpu.SemaphoreType.DMA,
            pltpu.SemaphoreType.DMA((4,)),
            pltpu.SemaphoreType.DMA((PACED + len(BULK_STARTS),)),
            pltpu.SemaphoreType.DMA((12,)),
            pltpu.SemaphoreType.DMA((12,)),
        ],
        compiler_params=pltpu.CompilerParams(
            collective_id=0, has_side_effects=True, vmem_limit_bytes=60 * 1024 * 1024
        ),
        name="decode",
    )(
        lengths,
        page_owner,
        page_index,
        page_dest,
        page_dest.reshape(N_DEV * PG_DEV // HD, HD),
        src_cache,
        queries.reshape(ROWS, HQ * HD),
        new_kv,
        hidden_in.reshape(ROWS, 32),
        out_weight.T,
        norm_gain.reshape(1, 32),
        router.T,
        routes.transpose(0, 2, 1),
        w_gate[0],
        w_up[0],
        w_down[0],
    )
    page_pool, mixed = pl.pallas_call(
        finish_kernel,
        out_shape=(
            jax.ShapeDtypeStruct((SLOTS_DEV, PAGE, 2 * HD), BF16),
            jax.ShapeDtypeStruct((2, REQS, 32), BF16),
        ),
        in_specs=[vmem, vmem],
        out_specs=(hbm, hbm),
        scratch_shapes=[pltpu.SemaphoreType.DMA((7,))],
        compiler_params=pltpu.CompilerParams(vmem_limit_bytes=1024 * 1024),
        name="finish",
    )(
        pltpu.with_memory_space_constraint(page_pool, pltpu.VMEM),
        pltpu.with_memory_space_constraint(mixed, pltpu.VMEM),
    )
    return (page_pool[None], mixed)


def solution(mesh):
    in_specs = (
        P(),
        P(),
        P(),
        P(),
        P(SEQ_HEAD, None, None, None),
        P(),
        P(),
        P(None, None, SEQ_HEAD),
        P(None, SEQ_HEAD),
        P(SEQ_HEAD),
        P(SEQ_HEAD, None),
        P(),
        P("seq", None, "head"),
        P("seq", None, "head"),
        P("seq", "head", None),
    )
    out_specs = (P("head", "seq", None, None), P(None, None, SEQ_HEAD))
    return jax.shard_map(body, mesh=mesh, in_specs=in_specs, out_specs=out_specs, check_vma=False)
```
